32 devices in a mesh: replica: 8 (over z, y), tensor: 4 (over x, core).
Axes of the slice: x: 2, y: 2, z: 4, core: 2. Of those that a mesh axis runs over, the one named last changes fastest.
Arguments:
- base_stream: bfloat16 [32, 8192], P('tensor', 'replica'), may hold values from -6 to 6
- out_weight: bfloat16 [64, 128, 8192], P('tensor', 'replica'), may hold values from -0.5 to 0.5
- queries: bfloat16 [4, 32, 64, 128], P(None, 'replica', 'tensor'), may hold values from -5 to 5
- cache_keys: bfloat16 [32, 8, 1536, 128], P('replica', 'tensor'), may hold values from -5 to 5
- cache_values: bfloat16 [32, 8, 1536, 128], P('replica', 'tensor'), may hold values from -6 to 6
- new_keys: bfloat16 [4, 32, 8, 128], P(None, 'replica', 'tensor'), may hold values from -5 to 5
- new_values: bfloat16 [4, 32, 8, 128], P(None, 'replica', 'tensor'), may hold values from -6 to 6
- lengths: int32 [32], P('replica'), may hold values from 384 to 1536
- finished: int32 [32], replicated, may hold values 0 or 1
- owners: int32 [32, 1], replicated, may hold values from 0 to 7; in each aligned block of 32 rows (0 to 31, 32 to 63, ...) at most 4 rows name the same one
Outputs:
- updates: bfloat16 [4, 32, 8192], P(None, 'tensor', 'replica')
- trainer_rows: bfloat16 [8, 4, 8192], P('replica', 'tensor')
The draws below stay inside these ranges and needn't reach their ends.
Inputs may be any that keep to these rules, and one draw needn't show every extreme that they name: `owners`: no owner is named by more than 4 rows, and one owner is named by exactly 4.
All inputs are finite; a program needn't handle non-finite values.
Results may differ from the reference program's by a relative error of at most 0.013.
Values may be sent and summed in bfloat16 or wider, within the bound.
No kernel may reach another device: no remote copies, remote signals or barrier semaphores. Data moves between devices by JAX's collectives and lax.ppermute only.
A program may use at most 128 MiB of HBM per device.

```python
import math
import jax
import jax.numpy as jnp
import numpy as np
from jax import lax

D = 8192
QH = 64
KVH = 8
HD = 128
ROW_DEV = 4
CTX = 1536
STEPS = 4
ROWS = 32
CAP = 4
N_REPLICA = 8
N_TENSOR = 4


def shared_parts(key):
    base = jax.random.fold_in(key, 1234)
    key_common = jax.random.fold_in(base, 0)
    common = jax.random.normal(key_common, (STEPS, ROWS, KVH, HD), jnp.float32)
    return common


def draw_queries(key, part):
    common = shared_parts(key)
    group_size = QH // KVH
    own_part = jax.random.normal(jax.random.fold_in(key, 21), (STEPS, ROWS, QH, HD), jnp.float32)
    values = jnp.clip(jnp.repeat(common, group_size, axis=2) + 0.6 * own_part, -5.0, 5.0)
    return values.astype(jnp.bfloat16)


def draw_cache_keys(key, part):
    values = jnp.clip(jax.random.normal(jax.random.fold_in(key, 31), (ROWS, KVH, CTX, HD), jnp.float32), -5.0, 5.0)
    return values.astype(jnp.bfloat16)


def draw_new_keys(key, part):
    common = shared_parts(key)
    noise = jax.random.normal(jax.random.fold_in(key, 41), (STEPS, ROWS, KVH, HD), jnp.float32)
    values = jnp.clip(0.4 * common + 0.7 * noise, -5.0, 5.0)
    return values.astype(jnp.bfloat16)


def touch_ends(values, key, least, top_value):
    shape = values.shape
    spot = [jax.random.randint(jax.random.fold_in(key, axis), (), 0, shape[axis]) for axis in range(len(shape))]
    values = values.at[tuple(spot)].set(least)
    longest = shape.index(max(shape))
    spot[longest] = (spot[longest] + 1) % shape[longest]
    return values.at[tuple(spot)].set(top_value)


def levels(rng, extent, pieces, low, top_value):
    level, own = 1.0, jax.random.fold_in(rng, 6)
    for dim, shards_of in pieces:
        heights = jnp.exp(jax.random.uniform(jax.random.fold_in(own, dim), (shards_of,), jnp.float32, low / len(pieces), top_value / len(pieces)))
        level = level * jnp.repeat(heights, extent[dim] // shards_of).reshape([-1 if axis == dim else 1 for axis in range(len(extent))])
    return level


def shared_out(stream_key, own, number, rows, amount, top, most, skew):
    ranking = jax.random.permutation(stream_key, amount)
    heavy_load, ordinary = portions_of(amount, rows * top, most, skew, True), portions_of(amount, rows * top, most, skew, False)
    places = jnp.arange(amount)

    def named(tallies, offset_by):
        used = int((tallies > 0).sum())
        fixed = max(1, used // 4)
        shifted = fixed + (places - fixed + offset_by * (used - fixed)) % max(1, amount - fixed)
        return jnp.zeros((amount,), jnp.int32).at[ranking[jnp.where(places < fixed, places, shifted)]].set(jnp.asarray(tallies, jnp.int32))

    tallies = jnp.where(number % 4 == 0, named(heavy_load, number // 4), named(ordinary, number - number // 4 - 1))
    mixed = jax.random.permutation(jax.random.fold_in(own, 3), amount)
    donor, taker = mixed[0:amount // 2 * 2:2], mixed[1:amount // 2 * 2:2]
    slack = jnp.minimum(tallies[donor] - 1, most - tallies[taker]) // 2
    slack = jnp.where((donor == ranking[0]) | (taker == ranking[0]) | (tallies[taker] == 0), 0, jnp.maximum(slack, 0))
    shifted = jax.random.randint(jax.random.fold_in(own, 4), (amount // 2,), 0, 1 << 20) % (slack + 1)
    tallies = tallies.at[donor].add(-shifted).at[taker].add(shifted)
    members = jnp.searchsorted(jnp.cumsum(tallies), jnp.arange(rows * top), side="right").astype(jnp.int32)
    listing = members.reshape(top, rows).T
    listing = listing[jax.random.permutation(jax.random.fold_in(own, 1), rows)]
    offset_by = jax.random.randint(jax.random.fold_in(own, 2), (rows, 1), 0, top)
    return jnp.take_along_axis(listing, (jnp.arange(top)[None, :] + offset_by) % top, axis=1)


def portions_of(number_of, total, reach, lean, full):
    portions = [(1 << 20) // math.isqrt(grade ** lean) + 1 for grade in range(1, number_of + 1)]
    largest = reach if full else min(reach, max(-(-total // number_of), total * portions[0] // sum(portions)))
    least = 1 if total - largest >= number_of - 1 else 0
    holding, rest = [largest] + [least] * (number_of - 1), total - largest - least * (number_of - 1)
    while rest > 0:
        movable = [i for i in range(1, number_of) if holding[i] < largest] or [i for i in range(1, number_of) if holding[i] < reach]
        whole, budget = sum([portions[i] for i in movable]), rest
        for i in movable:
            addition = min(reach - holding[i], max(1, budget * portions[i] // whole), rest)
            holding[i] = holding[i] + addition
            rest = rest - addition
    return np.array(holding)


def normal_values(own_key, extent, deviation, limit, pieces=(), kind=jnp.bfloat16):
    result = deviation * jax.random.normal(own_key, extent, jnp.float32)
    if pieces:
        result = result * levels(own_key, extent, pieces, -0.22, 0.18)
    return jnp.clip(result, -limit, limit).astype(kind)


def setup_inputs(seed: int = 0) -> dict:
    splits = jax.random.split(jax.random.key(seed), 11)
    base_stream = normal_values(splits[0], (ROWS, D), 1.0, 6.0, ((0, 4), (1, 8)))
    out_weight = normal_values(splits[1], (QH, HD, D), HD ** -0.5, 0.5, ((0, 4), (1, 8)))
    queries = draw_queries(jax.random.fold_in(splits[10], 71), 0)
    cache_keys = draw_cache_keys(jax.random.fold_in(splits[10], 71), 0)
    cache_values = normal_values(splits[4], (ROWS, KVH, CTX, HD), 1.0, 6.0, ((0, 8), (1, 4)))
    new_keys = draw_new_keys(jax.random.fold_in(splits[10], 71), 0)
    new_values = normal_values(splits[6], (STEPS, ROWS, KVH, HD), 1.0, 6.0, ((1, 8), (2, 4)))
    lengths = touch_ends(jax.random.randint(splits[7], (ROWS,), CTX // 4, CTX + 1), jax.random.fold_in(splits[7], 1), CTX // 4, CTX).astype(jnp.int32)
    finished = touch_ends((jax.random.randint(splits[8], (ROWS,), 0, 4) < 3).astype(jnp.int32), jax.random.fold_in(splits[8], 1), 0, 1)
    owners_keys = jax.random.split(jax.random.fold_in(splits[9], 1), ROWS // ROWS)
    owners_turns = jax.random.permutation(jax.random.fold_in(splits[9], 3), ROWS // ROWS)
    owners = jax.vmap(lambda own, number: shared_out(jax.random.fold_in(splits[9], 2), own, number, ROWS, N_REPLICA, 1, CAP, 2))(owners_keys, owners_turns).reshape((ROWS, 1))
    return dict(base_stream=base_stream, out_weight=out_weight, queries=queries, cache_keys=cache_keys, cache_values=cache_values, new_keys=new_keys, new_values=new_values, lengths=lengths, finished=finished, owners=owners)


def attend_block(block):
    query_rows, key_rows, value_rows, fresh_keys, fresh_values, row_lengths = block
    group_size = QH // KVH
    count = query_rows.shape[1]
    score_scale = 1.0 / math.sqrt(HD)
    grouped = query_rows.astype(jnp.float32).reshape(STEPS, count, KVH, group_size, HD)
    cache_scores = jnp.einsum('tbgqd,bgcd->tbgqc', grouped, key_rows.astype(jnp.float32)) * score_scale
    positions = lax.broadcasted_iota(jnp.int32, (1, count, 1, 1, CTX), 4)
    is_valid = positions < row_lengths.astype(jnp.int32)[None, :, None, None, None]
    cache_scores = jnp.where(is_valid, cache_scores, jnp.float32(-1e+30))
    fresh_scores = jnp.einsum('tbgqd,ubgd->tbgqu', grouped, fresh_keys.astype(jnp.float32)) * score_scale
    step_now = lax.broadcasted_iota(jnp.int32, (STEPS, 1, 1, 1, STEPS), 0)
    step_then = lax.broadcasted_iota(jnp.int32, (STEPS, 1, 1, 1, STEPS), 4)
    fresh_scores = jnp.where(step_then <= step_now, fresh_scores, jnp.float32(-1e+30))
    highest = jnp.maximum(lax.optimization_barrier(jnp.max(cache_scores, axis=-1, keepdims=True)), lax.optimization_barrier(jnp.max(fresh_scores, axis=-1, keepdims=True)))
    cache_weights = jnp.exp(cache_scores - highest)
    fresh_weights = jnp.exp(fresh_scores - highest)
    totals = lax.optimization_barrier(jnp.sum(cache_weights, axis=-1, keepdims=True)) + lax.optimization_barrier(jnp.sum(fresh_weights, axis=-1, keepdims=True))
    cache_probs = (cache_weights / totals).astype(jnp.bfloat16).astype(jnp.float32)
    fresh_probs = (fresh_weights / totals).astype(jnp.bfloat16).astype(jnp.float32)
    mixed = jnp.einsum('tbgqc,bgcd->tbgqd', cache_probs, value_rows.astype(jnp.float32))
    mixed = mixed + jnp.einsum('tbgqu,ubgd->tbgqd', fresh_probs, fresh_values.astype(jnp.float32))
    return mixed.reshape(STEPS, count, QH * HD).astype(jnp.bfloat16)

def reference(base_stream, out_weight, queries, cache_keys, cache_values, new_keys, new_values, lengths, finished, owners):
    block_rows = ROW_DEV
    blocks = ROWS // block_rows
    query_blocks = queries.reshape(STEPS, blocks, block_rows, QH, HD).transpose(1, 0, 2, 3, 4)
    key_blocks = cache_keys.reshape(blocks, block_rows, KVH, CTX, HD)
    value_blocks = cache_values.reshape(blocks, block_rows, KVH, CTX, HD)
    fresh_key_blocks = new_keys.reshape(STEPS, blocks, block_rows, KVH, HD).transpose(1, 0, 2, 3, 4)
    fresh_value_blocks = new_values.reshape(STEPS, blocks, block_rows, KVH, HD).transpose(1, 0, 2, 3, 4)
    length_blocks = lengths.reshape(blocks, block_rows)
    attended = lax.map(attend_block, (query_blocks, key_blocks, value_blocks, fresh_key_blocks, fresh_value_blocks, length_blocks))
    attended = attended.transpose(1, 0, 2, 3).reshape(STEPS * ROWS, QH * HD)
    weight_flat = out_weight.reshape(QH * HD, D)
    group_width = QH // N_TENSOR * HD
    projected = jnp.zeros((STEPS * ROWS, D), jnp.float32)
    for group in range(N_TENSOR):
        lower = group * group_width
        upper = lower + group_width
        partial_value = jnp.dot(attended[:, lower:upper], weight_flat[lower:upper], preferred_element_type=jnp.float32)
        rounded = lax.optimization_barrier(partial_value.astype(jnp.bfloat16))
        projected = projected + rounded.astype(jnp.float32)
    updates = projected.reshape(STEPS, ROWS, D).astype(jnp.bfloat16)
    stream = base_stream.astype(jnp.float32) + lax.optimization_barrier(jnp.sum(updates.astype(jnp.float32), axis=0))
    owner_ids = lax.broadcasted_iota(jnp.int32, (1, N_REPLICA), 1)
    onehot = (owners.astype(jnp.int32) == owner_ids).astype(jnp.int32)
    running = jnp.cumsum(onehot, axis=0)
    slot_rank = lax.optimization_barrier(jnp.sum((running - onehot) * onehot, axis=1)).astype(jnp.int32)
    slot_index = (owners[:, 0].astype(jnp.int32) * CAP + slot_rank).astype(jnp.int32)
    handed = stream.astype(jnp.bfloat16) * finished.astype(jnp.bfloat16)[:, None]
    buffer = jnp.zeros((N_REPLICA * CAP, D), jnp.bfloat16).at[slot_index].set(handed)
    trainer_rows = buffer.reshape(N_REPLICA, CAP, D)
    return (updates, trainer_rows)
```

```python
import functools
import math

import jax
import jax.numpy as jnp
from jax import lax
from jax.experimental import pallas as pl
from jax.experimental.pallas import tpu as pltpu
from jax.sharding import PartitionSpec as P

SLOT_DEV = 1
LANES = 128


def attend(queries, cache_keys, cache_values, new_keys, new_values, lengths):
    steps_count, row_count, heads_here, head_size = queries.shape
    kv_here = cache_keys.shape[1]
    positions_count = cache_keys.shape[2]
    group_size = heads_here // kv_here
    score_scale = 1.0 / math.sqrt(head_size)
    grouped = queries.reshape(steps_count, row_count, kv_here, group_size, head_size)
    cache_scores = (
        jnp.einsum("tbgqd,bgcd->tbgqc", grouped, cache_keys, preferred_element_type=jnp.float32)
        * score_scale
    )
    positions = lax.broadcasted_iota(jnp.int32, (1, row_count, 1, 1, positions_count), 4)
    is_valid = positions < lengths[None, :, None, None, None]
    cache_scores = jnp.where(is_valid, cache_scores, jnp.float32(-1e30))
    fresh_scores = (
        jnp.einsum("tbgqd,ubgd->tbgqu", grouped, new_keys, preferred_element_type=jnp.float32)
        * score_scale
    )
    step_now = lax.broadcasted_iota(jnp.int32, (steps_count, 1, 1, 1, steps_count), 0)
    step_then = lax.broadcasted_iota(jnp.int32, (steps_count, 1, 1, 1, steps_count), 4)
    fresh_scores = jnp.where(step_then <= step_now, fresh_scores, jnp.float32(-1e30))
    highest = jnp.maximum(
        jnp.max(cache_scores, axis=-1, keepdims=True), jnp.max(fresh_scores, axis=-1, keepdims=True)
    )
    cache_weights = jnp.exp(cache_scores - highest)
    fresh_weights = jnp.exp(fresh_scores - highest)
    totals = jnp.sum(cache_weights, axis=-1, keepdims=True) + jnp.sum(
        fresh_weights, axis=-1, keepdims=True
    )
    cache_probs = (cache_weights / totals).astype(jnp.bfloat16)
    fresh_probs = (fresh_weights / totals).astype(jnp.bfloat16)
    mixed = jnp.einsum(
        "tbgqc,bgcd->tbgqd", cache_probs, cache_values, preferred_element_type=jnp.float32
    )
    mixed = mixed + jnp.einsum(
        "tbgqu,ubgd->tbgqd", fresh_probs, new_values, preferred_element_type=jnp.float32
    )
    return mixed.reshape(steps_count, row_count, heads_here * head_size).astype(jnp.bfloat16)


def reduce_heads(partial_value):
    rounded = partial_value.astype(jnp.bfloat16)
    totals = lax.psum(rounded, "tensor").astype(jnp.float32)
    share = totals.shape[1] // lax.axis_size("tensor")
    return lax.dynamic_slice_in_dim(totals, lax.axis_index("tensor") * share, share, 1)


def regroup_weight(
    base_stream,
    out_weight,
    queries,
    cache_keys,
    cache_values,
    new_keys,
    new_values,
    lengths,
    finished,
    owners,
):
    heads_here = out_weight.shape[0]
    regrouped = lax.all_to_all(out_weight, "replica", split_axis=2, concat_axis=1, tiled=True)
    weight_local = regrouped.reshape(heads_here * regrouped.shape[1], regrouped.shape[2])
    attended = attend(queries, cache_keys, cache_values, new_keys, new_values, lengths)
    partial_value = jnp.einsum(
        "tbf,fc->tbc",
        lax.all_gather(attended, "replica", axis=1, tiled=True),
        weight_local,
        preferred_element_type=jnp.float32,
    )
    summed = reduce_heads(partial_value)
    updates = summed.astype(jnp.bfloat16)
    stream = base_stream.astype(jnp.float32) + jnp.sum(updates.astype(jnp.float32), axis=0)
    stream_rounded = stream.astype(jnp.bfloat16)
    all_streams = lax.all_gather(stream_rounded, "tensor", axis=0, tiled=True)
    owner_count = lax.axis_size("replica")
    owner_ids = lax.broadcasted_iota(jnp.int32, (1, owner_count), 1)
    onehot = (owners == owner_ids).astype(jnp.int32)
    before = jnp.cumsum(onehot, axis=0) - onehot
    slot_rank = jnp.sum(before * onehot, axis=1)
    first_slot = lax.axis_index("tensor") * SLOT_DEV
    slot_ids = first_slot + lax.broadcasted_iota(jnp.int32, (1, 1, SLOT_DEV), 2)
    chosen = (
        onehot[:, :, None]
        * (slot_rank[:, None, None] == slot_ids).astype(jnp.int32)
        * finished[:, None, None]
    )
    selector = chosen.astype(jnp.bfloat16)
    outgoing = jnp.einsum(
        "jos,jc->osc", selector, all_streams, preferred_element_type=jnp.float32
    ).astype(jnp.bfloat16)
    trainer_rows = lax.all_to_all(outgoing, "replica", split_axis=0, concat_axis=2, tiled=True)
    return (updates, trainer_rows)


def select_rows(owners, finished, steps_count, row_count, columns):
    replicas, tensors = lax.axis_size("replica"), lax.axis_size("tensor")
    me_r, me_t = lax.axis_index("replica"), lax.axis_index("tensor")
    total_rows = replicas * row_count
    share = total_rows // tensors
    width = steps_count * total_rows
    shape = (tensors, steps_count * share, width)
    col = lax.broadcasted_iota(jnp.int32, shape, 2)
    col_row = col // (steps_count * row_count) * row_count + col % row_count
    col_step = col // row_count % steps_count
    target = lax.broadcasted_iota(jnp.int32, shape, 0) ^ me_t
    line = lax.broadcasted_iota(jnp.int32, shape, 1)
    update_rows = (col_row == target * share + line % share) & (col_step == line // share)
    names = owners[:, 0]
    index = jnp.arange(total_rows)
    rank = jnp.sum((names[None, :] == names[:, None]) & (index[None, :] < index[:, None]), axis=1)
    spread = lambda v: jnp.broadcast_to(
        v.reshape(replicas, 1, row_count), (replicas, steps_count, row_count)
    ).reshape(1, 1, width)
    shape = (tensors, replicas, width)
    slot = lax.broadcasted_iota(jnp.int32, shape, 0) ^ me_t
    owner = lax.broadcasted_iota(jnp.int32, shape, 1) ^ me_r
    slot_rows = (spread(names) == owner) & (spread(rank) == slot) & (spread(finished) > 0)
    rows = jnp.concatenate([update_rows, slot_rows], axis=1)
    own = lax.broadcasted_iota(jnp.int32, (1, 1, share), 2) + me_t * share
    pick = lambda v: lax.dynamic_slice_in_dim(v, me_t * share, share).reshape(1, 1, share)
    base_rows = (pick(names) == owner[:, :, :share]) & (pick(rank) == slot[:, :, :share]) & (
        pick(finished) > 0
    )
    return (
        rows.reshape(-1, width).astype(jnp.bfloat16),
        base_rows.reshape(-1, share).astype(jnp.bfloat16),
    )


def project_kernel(
    sizes, me_ref, gathered, rows, base_rows, base, weight, *refs
):
    tensors, replicas, lines, slots = sizes
    outs, (held, slot_sums) = refs[:-2], refs[-2:]
    step = pl.program_id(0)
    me = me_ref[0]

    @pl.when(step == 0)
    def _():
        held[...] = jnp.dot(
            rows[...], gathered[...], preferred_element_type=jnp.float32
        ).astype(jnp.bfloat16)

    block = step ^ me
    sums = jnp.dot(held[...], weight[...], preferred_element_type=jnp.float32)
    cols = sums.shape[1]
    half = cols // 2
    low, high = step % 2, step // 2
    for t in range(tensors):
        first = t * (lines + slots)
        part = sums[first : first + lines].astype(jnp.bfloat16)
        a_ref, b_ref = outs[t % 2], outs[2 + t % 2]
        a_ref[t // 2, low, high, :lines] = part[:, :half]
        b_ref[low, t // 2, high, :lines] = part[:, half:]
        for c in range(cols // LANES):
            slot_sums[t, c, pl.ds(block, slots, stride=replicas), :] = sums[
                first + lines : first + lines + slots, c * LANES : (c + 1) * LANES
            ]

    @pl.when(step == 0)
    def _():
        extra = jnp.dot(base_rows[...], base[...], preferred_element_type=jnp.float32)
        for t in range(tensors):
            for c in range(cols // LANES):
                slot_sums[t, c, pl.ds(me, slots, stride=replicas), :] += extra[
                    t * slots : (t + 1) * slots, c * LANES : (c + 1) * LANES
                ]

    @pl.when(step == pl.num_programs(0) - 1)
    def _():
        for t in range(tensors):
            a_ref, b_ref = outs[t % 2], outs[2 + t % 2]
            for r in range(replicas):
                for c in range(cols // LANES):
                    part = slot_sums[t, c, r * replicas : (r + 1) * replicas].astype(jnp.bfloat16)
                    at = c * LANES % half
                    if c * LANES < half:
                        a_ref[t // 2, r % 2, r // 2, lines:, at : at + LANES] = part
                    else:
                        b_ref[r % 2, t // 2, r // 2, lines:, at : at + LANES] = part


def project(gathered, rows, base_rows, base_stream, weight):
    replicas, tensors = lax.axis_size("replica"), lax.axis_size("tensor")
    depth, model = weight.shape
    cols = model // replicas
    slots = replicas
    lines = rows.shape[0] // tensors - slots
    me = lax.axis_index("replica").astype(jnp.int32).reshape(1)
    whole = lambda v: pl.BlockSpec(v.shape, lambda j, me: (0,) * v.ndim)
    a_shape = (tensors // 2, 2, replicas // 2, lines + replicas, cols // 2)
    b_shape = (2, tensors // 2, replicas // 2, lines + replicas, cols // 2)
    shapes = [jax.ShapeDtypeStruct(s, jnp.bfloat16) for s in (a_shape, a_shape, b_shape, b_shape)]
    return pl.pallas_call(
        functools.partial(project_kernel, (tensors, replicas, lines, slots)),
        out_shape=shapes,
        grid_spec=pltpu.PrefetchScalarGridSpec(
            num_scalar_prefetch=1,
            grid=(replicas,),
            in_specs=[
                whole(gathered),
                whole(rows),
                whole(base_rows),
                whole(base_stream),
                pl.BlockSpec((depth, cols), lambda j, me: (0, j ^ me[0])),
            ],
            out_specs=[whole(s) for s in shapes],
            scratch_shapes=[
                pltpu.VMEM((rows.shape[0], depth), jnp.bfloat16),
                pltpu.VMEM((tensors, cols // LANES, slots * replicas, LANES), jnp.float32),
            ],
        ),
        cost_estimate=pl.CostEstimate(
            flops=2 * rows.shape[0] * depth * model,
            bytes_accessed=2 * depth * model,
            transcendentals=0,
        ),
        name="project",
    )(me, gathered, rows, base_rows, base_stream, weight)


def exchange(value, axis, mask):
    size = lax.axis_size(axis)
    return lax.ppermute(value, axis, [(i, i ^ mask) for i in range(size)])


def fold(value, axis, bit):
    came = exchange(value[1].astype(jnp.bfloat16), axis, bit)
    return value[0] + came.astype(jnp.float32)


def move_sums(
    base_stream,
    out_weight,
    queries,
    cache_keys,
    cache_values,
    new_keys,
    new_values,
    lengths,
    finished,
    owners,
):
    steps_count, row_count, heads_here, head_size = queries.shape
    replicas, tensors = lax.axis_size("replica"), lax.axis_size("tensor")
    feats = out_weight.shape[1]
    depth = heads_here * feats
    model = out_weight.shape[2]
    cols = model // replicas
    share = replicas * row_count // tensors
    lines = steps_count * share
    attended = attend(queries, cache_keys, cache_values, new_keys, new_values, lengths)
    split = attended.reshape(steps_count * row_count, heads_here, replicas, feats)
    split = split.transpose(2, 0, 1, 3).reshape(replicas, steps_count * row_count, depth)
    gathered = lax.all_to_all(split, "replica", split_axis=0, concat_axis=0, tiled=True)
    gathered = gathered.reshape(replicas * steps_count * row_count, depth)
    rows, base_rows = select_rows(owners, finished, steps_count, row_count, cols)
    weight = out_weight.reshape(depth, model)
    a_keep, a_send, b_keep, b_send = project(gathered, rows, base_rows, base_stream, weight)
    f32 = jnp.float32
    a_sum = a_keep.astype(f32) + exchange(a_send, "tensor", 1).astype(f32)
    b_sum = b_keep.astype(f32) + exchange(b_send, "tensor", 1).astype(f32)
    a_sum = fold(a_sum, "tensor", 2)
    b_sum = fold(b_sum, "replica", 1)
    a_sum = fold(a_sum, "replica", 1)
    b_sum = fold(b_sum, "tensor", 2)

    def last(value):
        total = value[0]
        for m in range(1, replicas // 2):
            total = total + exchange(value[m].astype(jnp.bfloat16), "replica", 2 * m).astype(f32)
        return total.astype(jnp.bfloat16)

    total = jnp.concatenate([last(a_sum), last(b_sum)], axis=1)
    updates = total[:lines].reshape(steps_count, share, cols)
    trainer_rows = total[lines:].reshape(1, SLOT_DEV, model)
    return (updates, trainer_rows)


def shards(*arrays):
    base_stream, out_weight, queries = arrays[:3]
    steps_count, row_count, heads_here, _ = queries.shape
    replicas, tensors = lax.axis_size("replica"), lax.axis_size("tensor")
    sent = steps_count * row_count * replicas
    few = sent <= heads_here * out_weight.shape[1]
    paired = tensors == 4 and replicas >= 4 and replicas & (replicas - 1) == 0
    return (move_sums if few and paired else regroup_weight)(*arrays)


def solution(mesh):
    placed = (
        P("tensor", "replica"),
        P("tensor", "replica", None),
        P(None, "replica", "tensor", None),
        P("replica", "tensor", None, None),
        P("replica", "tensor", None, None),
        P(None, "replica", "tensor", None),
        P(None, "replica", "tensor", None),
        P("replica"),
        P(),
        P(),
    )
    return jax.shard_map(
        shards,
        mesh=mesh,
        in_specs=placed,
        out_specs=(P(None, "tensor", "replica"), P("replica", "tensor", None)),
        check_vma=False,
    )
```

```python
import functools
import math

import jax
import jax.numpy as jnp
from jax import lax
from jax.experimental import pallas as pl
from jax.experimental.pallas import tpu as pltpu
from jax.sharding import PartitionSpec as P

SLOT_DEV = 1
LANES = 128


def attend(queries, cache_keys, cache_values, new_keys, new_values, lengths):
    steps_count, row_count, heads_here, head_size = queries.shape
    kv_here = cache_keys.shape[1]
    positions_count = cache_keys.shape[2]
    group_size = heads_here // kv_here
    score_scale = 1.0 / math.sqrt(head_size)
    grouped = queries.reshape(steps_count, row_count, kv_here, group_size, head_size)
    cache_scores = (
        jnp.einsum("tbgqd,bgcd->tbgqc", grouped, cache_keys, preferred_element_type=jnp.float32)
        * score_scale
    )
    positions = lax.broadcasted_iota(jnp.int32, (1, row_count, 1, 1, positions_count), 4)
    is_valid = positions < lengths[None, :, None, None, None]
    cache_scores = jnp.where(is_valid, cache_scores, jnp.float32(-1e30))
    fresh_scores = (
        jnp.einsum("tbgqd,ubgd->tbgqu", grouped, new_keys, preferred_element_type=jnp.float32)
        * score_scale
    )
    step_now = lax.broadcasted_iota(jnp.int32, (steps_count, 1, 1, 1, steps_count), 0)
    step_then = lax.broadcasted_iota(jnp.int32, (steps_count, 1, 1, 1, steps_count), 4)
    fresh_scores = jnp.where(step_then <= step_now, fresh_scores, jnp.float32(-1e30))
    highest = jnp.maximum(
        jnp.max(cache_scores, axis=-1, keepdims=True), jnp.max(fresh_scores, axis=-1, keepdims=True)
    )
    cache_weights = jnp.exp(cache_scores - highest)
    fresh_weights = jnp.exp(fresh_scores - highest)
    totals = jnp.sum(cache_weights, axis=-1, keepdims=True) + jnp.sum(
        fresh_weights, axis=-1, keepdims=True
    )
    cache_probs = (cache_weights / totals).astype(jnp.bfloat16)
    fresh_probs = (fresh_weights / totals).astype(jnp.bfloat16)
    mixed = jnp.einsum(
        "tbgqc,bgcd->tbgqd", cache_probs, cache_values, preferred_element_type=jnp.float32
    )
    mixed = mixed + jnp.einsum(
        "tbgqu,ubgd->tbgqd", fresh_probs, new_values, preferred_element_type=jnp.float32
    )
    return mixed.reshape(steps_count, row_count, heads_here * head_size).astype(jnp.bfloat16)


def reduce_heads(partial_value):
    rounded = partial_value.astype(jnp.bfloat16)
    totals = lax.psum(rounded, "tensor").astype(jnp.float32)
    share = totals.shape[1] // lax.axis_size("tensor")
    return lax.dynamic_slice_in_dim(totals, lax.axis_index("tensor") * share, share, 1)


def regroup_weight(
    base_stream,
    out_weight,
    queries,
    cache_keys,
    cache_values,
    new_keys,
    new_values,
    lengths,
    finished,
    owners,
):
    heads_here = out_weight.shape[0]
    regrouped = lax.all_to_all(out_weight, "replica", split_axis=2, concat_axis=1, tiled=True)
    weight_local = regrouped.reshape(heads_here * regrouped.shape[1], regrouped.shape[2])
    attended = attend(queries, cache_keys, cache_values, new_keys, new_values, lengths)
    partial_value = jnp.einsum(
        "tbf,fc->tbc",
        lax.all_gather(attended, "replica", axis=1, tiled=True),
        weight_local,
        preferred_element_type=jnp.float32,
    )
    summed = reduce_heads(partial_value)
    updates = summed.astype(jnp.bfloat16)
    stream = base_stream.astype(jnp.float32) + jnp.sum(updates.astype(jnp.float32), axis=0)
    stream_rounded = stream.astype(jnp.bfloat16)
    all_streams = lax.all_gather(stream_rounded, "tensor", axis=0, tiled=True)
    owner_count = lax.axis_size("replica")
    owner_ids = lax.broadcasted_iota(jnp.int32, (1, owner_count), 1)
    onehot = (owners == owner_ids).astype(jnp.int32)
    before = jnp.cumsum(onehot, axis=0) - onehot
    slot_rank = jnp.sum(before * onehot, axis=1)
    first_slot = lax.axis_index("tensor") * SLOT_DEV
    slot_ids = first_slot + lax.broadcasted_iota(jnp.int32, (1, 1, SLOT_DEV), 2)
    chosen = (
        onehot[:, :, None]
        * (slot_rank[:, None, None] == slot_ids).astype(jnp.int32)
        * finished[:, None, None]
    )
    selector = chosen.astype(jnp.bfloat16)
    outgoing = jnp.einsum(
        "jos,jc->osc", selector, all_streams, preferred_element_type=jnp.float32
    ).astype(jnp.bfloat16)
    trainer_rows = lax.all_to_all(outgoing, "replica", split_axis=0, concat_axis=2, tiled=True)
    return (updates, trainer_rows)


def attend_kernel(scale, lengths, queries, new_keys, new_values, keys, values, out, held, fresh_k, fresh_v, turned, sems):
    steps_count, row_count, heads_here, head_size = queries.shape
    kv_here, positions_count = keys.shape[1], keys.shape[2]
    group = heads_here // kv_here
    lines = steps_count * group
    f32 = jnp.float32
    fetches = [
        pltpu.make_async_copy(values.at[i], held.at[i], sems.at[i]) for i in range(row_count)
    ]
    for fetch in fetches:
        fetch.start()
    fresh_k[...] = jnp.zeros_like(fresh_k)
    fresh_v[...] = jnp.zeros_like(fresh_v)
    place = lax.broadcasted_iota(jnp.int32, (lines, positions_count), 1)
    fresh_at = lax.broadcasted_iota(jnp.int32, (lines, LANES), 1)
    fresh_step = lax.broadcasted_iota(jnp.int32, (lines, LANES), 0) // group
    fresh_valid = fresh_at <= fresh_step
    width = head_size // group
    lane = lax.broadcasted_iota(jnp.int32, (group, head_size), 1) // width
    diagonal = (lane - lax.broadcasted_iota(jnp.int32, (group, head_size), 0)) & (group - 1)
    turn = (((1,), (1,)), ((), ()))
    for i in range(row_count):
        is_valid = place < lengths[i]
        weighed = []
        for g in range(kv_here):
            query = jnp.concatenate(
                [queries[t, i, g * group : (g + 1) * group] for t in range(steps_count)], axis=0
            )
            for t in range(steps_count):
                fresh_k[g, t : t + 1] = new_keys[t, i, g : g + 1]
                fresh_v[g, t : t + 1] = new_values[t, i, g : g + 1]
            scores = lax.dot_general(query, keys[i, g], turn, preferred_element_type=f32) * scale
            scores = jnp.where(is_valid, scores, f32(-1e30))
            fresh = lax.dot_general(query, fresh_k[g], turn, preferred_element_type=f32) * scale
            fresh = jnp.where(fresh_valid, fresh, f32(-1e30))
            highest = jnp.maximum(
                jnp.max(scores, axis=1, keepdims=True), jnp.max(fresh, axis=1, keepdims=True)
            )
            scores = jnp.exp(scores - highest)
            fresh = jnp.exp(fresh - highest)
            total = jnp.sum(scores, axis=1, keepdims=True) + jnp.sum(fresh, axis=1, keepdims=True)
            share = 1.0 / total
            weighed.append(
                ((scores * share).astype(jnp.bfloat16), (fresh * share).astype(jnp.bfloat16))
            )
        fetches[i].wait()
        for g in range(kv_here):
            probs, fresh_probs = weighed[g]
            mixed = jnp.dot(probs, held[i, g], preferred_element_type=f32)
            mixed = mixed + jnp.dot(fresh_probs, fresh_v[g], preferred_element_type=f32)
            for t in range(steps_count):
                part = mixed[t * group : (t + 1) * group]
                moved = jnp.where(diagonal == 0, part, 0.0)
                for d in range(1, group):
                    rolled = pltpu.roll(pltpu.roll(part, group - d, 0), d * width, 1)
                    moved = jnp.where(diagonal == d, rolled, moved)
                turned[g, pl.ds(t * row_count + i, group, stride=steps_count * row_count), :] = moved
    for g in range(kv_here):
        out[:, g * head_size : (g + 1) * head_size] = turned[g].astype(jnp.bfloat16)


def in_vmem(*arrays):
    return [pltpu.with_memory_space_constraint(v, pltpu.VMEM) for v in arrays]


def attend_split(queries, cache_keys, cache_values, new_keys, new_values, lengths):
    steps_count, row_count, heads_here, head_size = queries.shape
    _, kv_here, positions_count, _ = cache_keys.shape
    group = heads_here // kv_here
    lines = steps_count * row_count
    vmem = pl.BlockSpec(memory_space=pltpu.VMEM)
    out = pl.pallas_call(
        functools.partial(attend_kernel, 1.0 / math.sqrt(head_size)),
        out_shape=pltpu.VMEM((group * lines, kv_here * head_size), jnp.bfloat16),
        in_specs=[
            pl.BlockSpec(memory_space=pltpu.SMEM),
            vmem,
            vmem,
            vmem,
            vmem,
            pl.BlockSpec(memory_space=pl.ANY),
        ],
        out_specs=vmem,
        scratch_shapes=[
            pltpu.VMEM(cache_values.shape, jnp.bfloat16),
            pltpu.VMEM((kv_here, LANES, head_size), jnp.bfloat16),
            pltpu.VMEM((kv_here, LANES, head_size), jnp.bfloat16),
            pltpu.VMEM((kv_here, group * lines, head_size), jnp.float32),
            pltpu.SemaphoreType.DMA((row_count,)),
        ],
        compiler_params=pltpu.CompilerParams(vmem_limit_bytes=16 * 2**20),
        cost_estimate=pl.CostEstimate(
            flops=4 * lines * heads_here * positions_count * head_size,
            bytes_accessed=4 * row_count * kv_here * positions_count * head_size,
            transcendentals=lines * heads_here * positions_count,
        ),
        name="attend",
    )(lengths, *in_vmem(queries, new_keys, new_values, cache_keys), cache_values)
    return out.reshape(group, lines, kv_here * head_size)


def select_kernel(sizes, me, owners, finished, rows, base_rows):
    tensors, replicas, steps_count, row_count = sizes
    total_rows = replicas * row_count
    share = total_rows // tensors
    lines = steps_count * share
    me_r, me_t = me[0], me[1]

    def tell(row_of):
        name, rank, done = (jnp.zeros_like(row_of) for _ in range(3))
        for j in range(total_rows):
            name = jnp.where(row_of == j, owners[j], name)
            done = jnp.where(row_of == j, finished[j], done)
        for j in range(total_rows):
            rank = rank + jnp.where((name == owners[j]) & (row_of > j), 1, 0)
        return jnp.where(done > 0, name, -1), rank

    width = steps_count * total_rows
    col = lax.broadcasted_iota(jnp.int32, (1, width), 1)
    per = steps_count * row_count
    row_of = col // per * row_count + (col & (row_count - 1))
    step_of = (col & (per - 1)) // row_count
    name, rank = tell(row_of)
    own = lax.broadcasted_iota(jnp.int32, (1, LANES), 1)
    base_name, base_rank = tell(own + me_t * share)
    base_name = jnp.where(own < share, base_name, -1)
    line = lax.broadcasted_iota(jnp.int32, (lines, width), 0)
    line_row, line_step = line & (share - 1), line // share
    owner = lax.broadcasted_iota(jnp.int32, (replicas, width), 0) ^ me_r
    base_owner = lax.broadcasted_iota(jnp.int32, (replicas, LANES), 0) ^ me_r
    picked = lambda hit: jnp.where(hit, 1.0, 0.0).astype(jnp.bfloat16)
    for t in range(tensors):
        target = me_t ^ t
        hit = (row_of == target * share + line_row) & (step_of == line_step)
        first = t * (lines + replicas)
        rows[first : first + lines] = picked(hit)
        hit = (name == owner) & (rank == target)
        rows[first + lines : first + lines + replicas] = picked(hit)
        hit = (base_name == base_owner) & (base_rank == target)
        base_rows[t * replicas : (t + 1) * replicas] = picked(hit)[:, :share]


def select_rows(owners, finished, steps_count, row_count):
    replicas, tensors = lax.axis_size("replica"), lax.axis_size("tensor")
    me = jnp.stack([lax.axis_index("replica"), lax.axis_index("tensor")]).astype(jnp.int32)
    share = replicas * row_count // tensors
    smem, vmem = pl.BlockSpec(memory_space=pltpu.SMEM), pl.BlockSpec(memory_space=pltpu.VMEM)
    height = tensors * (steps_count * share + replicas)
    return pl.pallas_call(
        functools.partial(select_kernel, (tensors, replicas, steps_count, row_count)),
        out_shape=(
            pltpu.VMEM((height, steps_count * replicas * row_count), jnp.bfloat16),
            pltpu.VMEM((tensors * replicas, share), jnp.bfloat16),
        ),
        in_specs=[smem, smem, smem],
        out_specs=[vmem, vmem],
        compiler_params=pltpu.CompilerParams(vmem_limit_bytes=4 * 2**20),
        cost_estimate=pl.CostEstimate(flops=10**6, bytes_accessed=10**5, transcendentals=0),
        name="select",
    )(me, owners[:, 0], finished)


def project_kernel(sizes, part, me_ref, gathered, rows, base_rows, base, weight, keep, send, slot_sums):
    tensors, replicas, lines = sizes
    f32 = jnp.float32
    me = me_ref[0]
    half = keep.shape[-1]
    held = jnp.dot(rows[...], gathered[...], preferred_element_type=f32).astype(jnp.bfloat16)
    tall = lines + replicas
    extra = jnp.dot(
        base_rows[...], base[:, part * half : (part + 1) * half], preferred_element_type=f32
    )

    def at(t, r):
        ref = send if t % 2 else keep
        return ref.at[(t // 2, r % 2, r // 2) if part == 0 else (r % 2, t // 2, r // 2)]

    for r in range(replicas):
        block = r ^ me
        first_col = pl.multiple_of((block * 2 + part) * half, half)
        sums = jnp.dot(held, weight[:, pl.ds(first_col, half)], preferred_element_type=f32)
        for t in range(tensors):
            first = t * tall
            at(t, r)[:lines] = sums[first : first + lines].astype(jnp.bfloat16)
            slot = sums[first + lines : first + tall]
            if r == 0:
                slot = slot + extra[t * replicas : (t + 1) * replicas]
            for c in range(half // LANES):
                slot_sums[t, c, pl.ds(block, replicas, stride=replicas), :] = slot[
                    :, c * LANES : (c + 1) * LANES
                ]
    for t in range(tensors):
        for r in range(replicas):
            for c in range(half // LANES):
                at(t, r)[lines:, c * LANES : (c + 1) * LANES] = slot_sums[
                    t, c, r * replicas : (r + 1) * replicas
                ].astype(jnp.bfloat16)


def project(part, gathered, rows, base_rows, base_stream, weight):
    replicas, tensors = lax.axis_size("replica"), lax.axis_size("tensor")
    depth, model = weight.shape
    half = model // replicas // 2
    tall = rows.shape[0] // tensors
    me = lax.axis_index("replica").astype(jnp.int32).reshape(1)
    lead = (tensors // 2, 2) if part == 0 else (2, tensors // 2)
    shape = pltpu.VMEM(lead + (replicas // 2, tall, half), jnp.bfloat16)
    smem, vmem = pl.BlockSpec(memory_space=pltpu.SMEM), pl.BlockSpec(memory_space=pltpu.VMEM)
    return pl.pallas_call(
        functools.partial(project_kernel, (tensors, replicas, tall - replicas), part),
        out_shape=(shape, shape),
        in_specs=[smem] + [vmem] * 5,
        out_specs=(vmem, vmem),
        scratch_shapes=[
            pltpu.VMEM((tensors, half // LANES, replicas * replicas, LANES), jnp.float32),
        ],
        compiler_params=pltpu.CompilerParams(vmem_limit_bytes=8 * 2**20),
        cost_estimate=pl.CostEstimate(
            flops=rows.shape[0] * depth * model,
            bytes_accessed=depth * model,
            transcendentals=0,
        ),
        name=f"project_{part}",
    )(me, *in_vmem(gathered, rows, base_rows, base_stream, weight))


def exchange(value, axis, mask):
    size = lax.axis_size(axis)
    return lax.ppermute(value, axis, [(i, i ^ mask) for i in range(size)])


def reduce_scatter(keep, send, stages):
    f32 = jnp.float32
    came = [exchange(send, *stages[0])]

    def part(*at):
        terms = [keep[at]] + [v[at[i:]] for i, v in enumerate(came)]
        return functools.reduce(jnp.add, [v.astype(f32) for v in terms])

    last = keep.shape[2]
    came.append(exchange(part(1).astype(jnp.bfloat16), *stages[1]))
    came.append(exchange(part(0, 1).astype(jnp.bfloat16), *stages[2]))
    moved = [
        exchange(part(0, 0, m).astype(jnp.bfloat16), stages[3][0], stages[3][1] * m)
        for m in range(1, last)
    ]
    result = functools.reduce(jnp.add, [part(0, 0, 0)] + [v.astype(f32) for v in moved])
    return result.astype(jnp.bfloat16)


def move_sums(
    base_stream,
    out_weight,
    queries,
    cache_keys,
    cache_values,
    new_keys,
    new_values,
    lengths,
    finished,
    owners,
):
    steps_count, row_count, heads_here, head_size = queries.shape
    replicas, tensors = lax.axis_size("replica"), lax.axis_size("tensor")
    model = out_weight.shape[2]
    share = replicas * row_count // tensors
    lines = steps_count * share
    split = attend_split(queries, cache_keys, cache_values, new_keys, new_values, lengths)
    gathered = lax.all_to_all(split, "replica", split_axis=0, concat_axis=0, tiled=True)
    gathered = gathered.reshape(-1, gathered.shape[2])
    rows, base_rows = select_rows(owners, finished, steps_count, row_count)
    weight = out_weight.reshape(-1, model)
    operands = (gathered, rows, base_rows, base_stream, weight)
    core, across = ("tensor", 1), ("tensor", 2)
    beside, along = ("replica", 1), ("replica", 2)
    total = jnp.concatenate(
        [
            reduce_scatter(*project(0, *operands), (core, across, beside, along)),
            reduce_scatter(*project(1, *operands), (core, beside, across, along)),
        ],
        axis=1,
    )
    updates = total[:lines].reshape(steps_count, share, model // replicas)
    trainer_rows = total[lines:].reshape(1, SLOT_DEV, model)
    return (updates, trainer_rows)


def shards(*arrays):
    out_weight, queries, cache_keys = arrays[1:4]
    steps_count, row_count, heads_here, head_size = queries.shape
    replicas, tensors = lax.axis_size("replica"), lax.axis_size("tensor")
    sent = steps_count * row_count * replicas
    few = sent <= heads_here * out_weight.shape[1]
    group = heads_here // cache_keys.shape[1]
    shares = replicas * row_count // tensors
    powers = all(n & (n - 1) == 0 for n in (replicas, steps_count, row_count, shares))
    fits = tensors == 4 and replicas == group == 8 and powers and head_size == LANES
    return (move_sums if few and fits else regroup_weight)(*arrays)


def solution(mesh):
    placed = (
        P("tensor", "replica"),
        P("tensor", "replica", None),
        P(None, "replica", "tensor", None),
        P("replica", "tensor", None, None),
        P("replica", "tensor", None, None),
        P(None, "replica", "tensor", None),
        P(None, "replica", "tensor", None),
        P("replica"),
        P(),
        P(),
    )
    return jax.shard_map(
        shards,
        mesh=mesh,
        in_specs=placed,
        out_specs=(P(None, "tensor", "replica"), P("replica", "tensor", None)),
        check_vma=False,
    )
```

```python
import functools
import math

import jax
import jax.numpy as jnp
from jax import lax
from jax.experimental import pallas as pl
from jax.experimental.pallas import tpu as pltpu
from jax.sharding import PartitionSpec as P

SLOT_DEV = 1
LANES = 128


def attend(queries, cache_keys, cache_values, new_keys, new_values, lengths):
    steps_count, row_count, heads_here, head_size = queries.shape
    kv_here = cache_keys.shape[1]
    positions_count = cache_keys.shape[2]
    group_size = heads_here // kv_here
    score_scale = 1.0 / math.sqrt(head_size)
    grouped = queries.reshape(steps_count, row_count, kv_here, group_size, head_size)
    cache_scores = (
        jnp.einsum("tbgqd,bgcd->tbgqc", grouped, cache_keys, preferred_element_type=jnp.float32)
        * score_scale
    )
    positions = lax.broadcasted_iota(jnp.int32, (1, row_count, 1, 1, positions_count), 4)
    is_valid = positions < lengths[None, :, None, None, None]
    cache_scores = jnp.where(is_valid, cache_scores, jnp.float32(-1e30))
    fresh_scores = (
        jnp.einsum("tbgqd,ubgd->tbgqu", grouped, new_keys, preferred_element_type=jnp.float32)
        * score_scale
    )
    step_now = lax.broadcasted_iota(jnp.int32, (steps_count, 1, 1, 1, steps_count), 0)
    step_then = lax.broadcasted_iota(jnp.int32, (steps_count, 1, 1, 1, steps_count), 4)
    fresh_scores = jnp.where(step_then <= step_now, fresh_scores, jnp.float32(-1e30))
    highest = jnp.maximum(
        jnp.max(cache_scores, axis=-1, keepdims=True), jnp.max(fresh_scores, axis=-1, keepdims=True)
    )
    cache_weights = jnp.exp(cache_scores - highest)
    fresh_weights = jnp.exp(fresh_scores - highest)
    totals = jnp.sum(cache_weights, axis=-1, keepdims=True) + jnp.sum(
        fresh_weights, axis=-1, keepdims=True
    )
    cache_probs = (cache_weights / totals).astype(jnp.bfloat16)
    fresh_probs = (fresh_weights / totals).astype(jnp.bfloat16)
    mixed = jnp.einsum(
        "tbgqc,bgcd->tbgqd", cache_probs, cache_values, preferred_element_type=jnp.float32
    )
    mixed = mixed + jnp.einsum(
        "tbgqu,ubgd->tbgqd", fresh_probs, new_values, preferred_element_type=jnp.float32
    )
    return mixed.reshape(steps_count, row_count, heads_here * head_size).astype(jnp.bfloat16)


def reduce_heads(partial_value):
    rounded = partial_value.astype(jnp.bfloat16)
    totals = lax.psum(rounded, "tensor").astype(jnp.float32)
    share = totals.shape[1] // lax.axis_size("tensor")
    return lax.dynamic_slice_in_dim(totals, lax.axis_index("tensor") * share, share, 1)


def regroup_weight(
    base_stream,
    out_weight,
    queries,
    cache_keys,
    cache_values,
    new_keys,
    new_values,
    lengths,
    finished,
    owners,
):
    heads_here = out_weight.shape[0]
    regrouped = lax.all_to_all(out_weight, "replica", split_axis=2, concat_axis=1, tiled=True)
    weight_local = regrouped.reshape(heads_here * regrouped.shape[1], regrouped.shape[2])
    attended = attend(queries, cache_keys, cache_values, new_keys, new_values, lengths)
    partial_value = jnp.einsum(
        "tbf,fc->tbc",
        lax.all_gather(attended, "replica", axis=1, tiled=True),
        weight_local,
        preferred_element_type=jnp.float32,
    )
    summed = reduce_heads(partial_value)
    updates = summed.astype(jnp.bfloat16)
    stream = base_stream.astype(jnp.float32) + jnp.sum(updates.astype(jnp.float32), axis=0)
    stream_rounded = stream.astype(jnp.bfloat16)
    all_streams = lax.all_gather(stream_rounded, "tensor", axis=0, tiled=True)
    owner_count = lax.axis_size("replica")
    owner_ids = lax.broadcasted_iota(jnp.int32, (1, owner_count), 1)
    onehot = (owners == owner_ids).astype(jnp.int32)
    before = jnp.cumsum(onehot, axis=0) - onehot
    slot_rank = jnp.sum(before * onehot, axis=1)
    first_slot = lax.axis_index("tensor") * SLOT_DEV
    slot_ids = first_slot + lax.broadcasted_iota(jnp.int32, (1, 1, SLOT_DEV), 2)
    chosen = (
        onehot[:, :, None]
        * (slot_rank[:, None, None] == slot_ids).astype(jnp.int32)
        * finished[:, None, None]
    )
    selector = chosen.astype(jnp.bfloat16)
    outgoing = jnp.einsum(
        "jos,jc->osc", selector, all_streams, preferred_element_type=jnp.float32
    ).astype(jnp.bfloat16)
    trainer_rows = lax.all_to_all(outgoing, "replica", split_axis=0, concat_axis=2, tiled=True)
    return (updates, trainer_rows)


def attend_kernel(scale, *refs):
    sources, out, places, (fresh_k, fresh_v, turned, sems) = refs[:6], refs[6], refs[7:13], refs[13:]
    lengths, queries, new_keys, new_values, keys, held = places
    steps_count, row_count, heads_here, head_size = queries.shape
    kv_here, positions_count = keys.shape[1], keys.shape[2]
    group = heads_here // kv_here
    lines = steps_count * group
    f32 = jnp.float32
    small = [pltpu.make_async_copy(sources[n], places[n], sems.at[n]) for n in range(4)]
    fetch = lambda n, i: pltpu.make_async_copy(
        sources[4 + n].at[i], places[4 + n].at[i], sems.at[4 + n * row_count + i]
    )
    fetches = [(fetch(0, i), fetch(1, i)) for i in range(row_count)]
    fetches[0][0].start()
    for copy in small:
        copy.start()
    fetches[0][1].start()
    for pair in fetches[1:]:
        pair[0].start()
        pair[1].start()
    fresh_k[...] = jnp.zeros_like(fresh_k)
    fresh_v[...] = jnp.zeros_like(fresh_v)
    place = lax.broadcasted_iota(jnp.int32, (lines, positions_count), 1)
    fresh_at = lax.broadcasted_iota(jnp.int32, (lines, LANES), 1)
    fresh_step = lax.broadcasted_iota(jnp.int32, (lines, LANES), 0) // group
    fresh_valid = fresh_at <= fresh_step
    width = head_size // group
    lane = lax.broadcasted_iota(jnp.int32, (group, head_size), 1) // width
    diagonal = (lane - lax.broadcasted_iota(jnp.int32, (group, head_size), 0)) & (group - 1)
    turn = (((1,), (1,)), ((), ()))
    for copy in small:
        copy.wait()
    for i in range(row_count):
        fetches[i][0].wait()
        is_valid = place < lengths[i]
        weighed = []
        for g in range(kv_here):
            query = jnp.concatenate(
                [queries[t, i, g * group : (g + 1) * group] for t in range(steps_count)], axis=0
            )
            for t in range(steps_count):
                fresh_k[g, t : t + 1] = new_keys[t, i, g : g + 1]
                fresh_v[g, t : t + 1] = new_values[t, i, g : g + 1]
            scores = lax.dot_general(query, keys[i, g], turn, preferred_element_type=f32) * scale
            scores = jnp.where(is_valid, scores, f32(-1e30))
            fresh = lax.dot_general(query, fresh_k[g], turn, preferred_element_type=f32) * scale
            fresh = jnp.where(fresh_valid, fresh, f32(-1e30))
            highest = jnp.maximum(
                jnp.max(scores, axis=1, keepdims=True), jnp.max(fresh, axis=1, keepdims=True)
            )
            scores = jnp.exp(scores - highest)
            fresh = jnp.exp(fresh - highest)
            total = jnp.sum(scores, axis=1, keepdims=True) + jnp.sum(fresh, axis=1, keepdims=True)
            share = 1.0 / total
            weighed.append(
                ((scores * share).astype(jnp.bfloat16), (fresh * share).astype(jnp.bfloat16))
            )
        fetches[i][1].wait()
        for g in range(kv_here):
            probs, fresh_probs = weighed[g]
            mixed = jnp.dot(probs, held[i, g], preferred_element_type=f32)
            mixed = mixed + jnp.dot(fresh_probs, fresh_v[g], preferred_element_type=f32)
            for t in range(steps_count):
                part = mixed[t * group : (t + 1) * group]
                moved = jnp.where(diagonal == 0, part, 0.0)
                for d in range(1, group):
                    rolled = pltpu.roll(pltpu.roll(part, group - d, 0), d * width, 1)
                    moved = jnp.where(diagonal == d, rolled, moved)
                turned[g, pl.ds(t * row_count + i, group, stride=steps_count * row_count), :] = moved
    for g in range(kv_here):
        out[:, g * head_size : (g + 1) * head_size] = turned[g].astype(jnp.bfloat16)


def in_vmem(*arrays):
    return [pltpu.with_memory_space_constraint(v, pltpu.VMEM) for v in arrays]


def attend_split(queries, cache_keys, cache_values, new_keys, new_values, lengths):
    steps_count, row_count, heads_here, head_size = queries.shape
    _, kv_here, positions_count, _ = cache_keys.shape
    group = heads_here // kv_here
    lines = steps_count * row_count
    operands = (lengths, queries, new_keys, new_values, cache_keys, cache_values)
    vmem = pl.BlockSpec(memory_space=pltpu.VMEM)
    (out,) = pl.pallas_call(
        functools.partial(attend_kernel, 1.0 / math.sqrt(head_size)),
        out_shape=(pltpu.VMEM((group * lines, kv_here * head_size), jnp.bfloat16),),
        in_specs=[pl.BlockSpec(memory_space=pltpu.HBM)] * len(operands),
        out_specs=(vmem,),
        scratch_shapes=[
            pltpu.SMEM(lengths.shape, lengths.dtype),
            *(pltpu.VMEM(v.shape, v.dtype) for v in operands[1:]),
            pltpu.VMEM((kv_here, LANES, head_size), jnp.bfloat16),
            pltpu.VMEM((kv_here, LANES, head_size), jnp.bfloat16),
            pltpu.VMEM((kv_here, group * lines, head_size), jnp.float32),
            pltpu.SemaphoreType.DMA((4 + 2 * row_count,)),
        ],
        compiler_params=pltpu.CompilerParams(vmem_limit_bytes=16 * 2**20),
        cost_estimate=pl.CostEstimate(
            flops=4 * lines * heads_here * positions_count * head_size,
            bytes_accessed=4 * row_count * kv_here * positions_count * head_size,
            transcendentals=lines * heads_here * positions_count,
        ),
        name="attend",
    )(*[pltpu.with_memory_space_constraint(v, pltpu.HBM) for v in operands])
    return out.reshape(group, lines, kv_here * head_size)


def fetch_weight(weight, held, sems, me, part, blocks):
    if not blocks:
        return []
    half = held.shape[1] // len(blocks)
    return [
        pltpu.make_async_copy(
            weight.at[:, pl.ds(pl.multiple_of(((r ^ me) * 2 + part) * half, half), half)],
            held.at[:, pl.ds(n * half, half)],
            sems.at[n],
        )
        for n, r in enumerate(blocks)
    ]


def select_kernel(sizes, me, owners, finished, weight, rows, base_rows, early, late, *sems):
    tensors, replicas, steps_count, row_count = sizes
    total_rows = replicas * row_count
    share = total_rows // tensors
    lines = steps_count * share
    me_r, me_t = me[0], me[1]
    blocks = range(replicas)
    fetches = fetch_weight(weight, early, sems[0], me_r, 1, blocks)
    fetches += fetch_weight(weight, late, sems[1], me_r, 0, blocks[: replicas // 2])
    for fetch in fetches:
        fetch.start()

    def tell(row_of):
        name, rank, done = (jnp.zeros_like(row_of) for _ in range(3))
        for j in range(total_rows):
            name = jnp.where(row_of == j, owners[j], name)
            done = jnp.where(row_of == j, finished[j], done)
        for j in range(total_rows):
            rank = rank + jnp.where((name == owners[j]) & (row_of > j), 1, 0)
        return jnp.where(done > 0, name, -1), rank

    width = steps_count * total_rows
    col = lax.broadcasted_iota(jnp.int32, (1, width), 1)
    per = steps_count * row_count
    row_of = col // per * row_count + (col & (row_count - 1))
    step_of = (col & (per - 1)) // row_count
    name, rank = tell(row_of)
    own = lax.broadcasted_iota(jnp.int32, (1, LANES), 1)
    base_name, base_rank = tell(own + me_t * share)
    base_name = jnp.where(own < share, base_name, -1)
    line = lax.broadcasted_iota(jnp.int32, (lines, width), 0)
    line_row, line_step = line & (share - 1), line // share
    owner = lax.broadcasted_iota(jnp.int32, (replicas, width), 0) ^ me_r
    base_owner = lax.broadcasted_iota(jnp.int32, (replicas, LANES), 0) ^ me_r
    picked = lambda hit: jnp.where(hit, 1.0, 0.0).astype(jnp.bfloat16)
    for t in range(tensors):
        target = me_t ^ t
        hit = (row_of == target * share + line_row) & (step_of == line_step)
        first = t * (lines + replicas)
        rows[first : first + lines] = picked(hit)
        hit = (name == owner) & (rank == target)
        rows[first + lines : first + lines + replicas] = picked(hit)
        hit = (base_name == base_owner) & (base_rank == target)
        base_rows[t * replicas : (t + 1) * replicas] = picked(hit)[:, :share]
    for fetch in fetches:
        fetch.wait()


def select_rows(owners, finished, weight, steps_count, row_count):
    replicas, tensors = lax.axis_size("replica"), lax.axis_size("tensor")
    me = jnp.stack([lax.axis_index("replica"), lax.axis_index("tensor")]).astype(jnp.int32)
    share = replicas * row_count // tensors
    smem, vmem = pl.BlockSpec(memory_space=pltpu.SMEM), pl.BlockSpec(memory_space=pltpu.VMEM)
    height = tensors * (steps_count * share + replicas)
    depth, model = weight.shape
    return pl.pallas_call(
        functools.partial(select_kernel, (tensors, replicas, steps_count, row_count)),
        out_shape=(
            pltpu.VMEM((height, steps_count * replicas * row_count), jnp.bfloat16),
            pltpu.VMEM((tensors * replicas, share), jnp.bfloat16),
            pltpu.VMEM((depth, model // 2), weight.dtype),
            pltpu.VMEM((depth, model // 4), weight.dtype),
        ),
        in_specs=[smem, smem, smem, pl.BlockSpec(memory_space=pltpu.HBM)],
        out_specs=[vmem] * 4,
        scratch_shapes=[
            pltpu.SemaphoreType.DMA((replicas,)),
            pltpu.SemaphoreType.DMA((replicas // 2,)),
        ],
        compiler_params=pltpu.CompilerParams(vmem_limit_bytes=4 * 2**20),
        cost_estimate=pl.CostEstimate(
            flops=10**6, bytes_accessed=2 * weight.size, transcendentals=0
        ),
        name="select",
    )(me, owners[:, 0], finished, weight)


def project_kernel(sizes, part, me_ref, weight, *refs):
    gathered, rows, base_rows, base, first_weight, keep, send, slot_sums, rest, sems = refs
    tensors, replicas, lines = sizes
    f32 = jnp.float32
    me = me_ref[0]
    half = keep.shape[-1]
    near = first_weight.shape[1] // half
    fetches = fetch_weight(weight, rest, sems, me, part, range(near, replicas))
    for fetch in fetches:
        fetch.start()
    held = jnp.dot(rows[...], gathered[...], preferred_element_type=f32).astype(jnp.bfloat16)
    tall = lines + replicas
    extra = jnp.dot(
        base_rows[...], base[:, part * half : (part + 1) * half], preferred_element_type=f32
    )

    def at(t, r):
        ref = send if t % 2 else keep
        return ref.at[(t // 2, r % 2, r // 2) if part == 0 else (r % 2, t // 2, r // 2)]

    for r in range(replicas):
        block = r ^ me
        if r < near:
            columns = first_weight[:, r * half : (r + 1) * half]
        else:
            fetches[r - near].wait()
            columns = rest[:, (r - near) * half : (r - near + 1) * half]
        sums = jnp.dot(held, columns, preferred_element_type=f32)
        for t in range(tensors):
            first = t * tall
            at(t, r)[:lines] = sums[first : first + lines].astype(jnp.bfloat16)
            slot = sums[first + lines : first + tall]
            if r == 0:
                slot = slot + extra[t * replicas : (t + 1) * replicas]
            for c in range(half // LANES):
                slot_sums[t, c, pl.ds(block, replicas, stride=replicas), :] = slot[
                    :, c * LANES : (c + 1) * LANES
                ]
    for t in range(tensors):
        for r in range(replicas):
            for c in range(half // LANES):
                at(t, r)[lines:, c * LANES : (c + 1) * LANES] = slot_sums[
                    t, c, r * replicas : (r + 1) * replicas
                ].astype(jnp.bfloat16)


def project(part, gathered, rows, base_rows, base_stream, first_weight, weight):
    replicas, tensors = lax.axis_size("replica"), lax.axis_size("tensor")
    depth, model = weight.shape
    half = model // replicas // 2
    missing = max(1, replicas - first_weight.shape[1] // half)
    tall = rows.shape[0] // tensors
    me = lax.axis_index("replica").astype(jnp.int32).reshape(1)
    lead = (tensors // 2, 2) if part == 0 else (2, tensors // 2)
    shape = pltpu.VMEM(lead + (replicas // 2, tall, half), jnp.bfloat16)
    smem, vmem = pl.BlockSpec(memory_space=pltpu.SMEM), pl.BlockSpec(memory_space=pltpu.VMEM)
    return pl.pallas_call(
        functools.partial(project_kernel, (tensors, replicas, tall - replicas), part),
        out_shape=(shape, shape),
        in_specs=[smem, pl.BlockSpec(memory_space=pltpu.HBM)] + [vmem] * 5,
        out_specs=(vmem, vmem),
        scratch_shapes=[
            pltpu.VMEM((tensors, half // LANES, replicas * replicas, LANES), jnp.float32),
            pltpu.VMEM((depth, missing * half), weight.dtype),
            pltpu.SemaphoreType.DMA((missing,)),
        ],
        compiler_params=pltpu.CompilerParams(vmem_limit_bytes=8 * 2**20),
        cost_estimate=pl.CostEstimate(
            flops=rows.shape[0] * depth * model,
            bytes_accessed=depth * model,
            transcendentals=0,
        ),
        name=f"project_{part}",
    )(me, weight, *in_vmem(gathered, rows, base_rows, base_stream, first_weight))


def exchange(value, axis, mask):
    size = lax.axis_size(axis)
    return lax.ppermute(value, axis, [(i, i ^ mask) for i in range(size)])


def add_up(terms):
    return functools.reduce(jnp.add, [v.astype(jnp.float32) for v in terms])


def part_of(keep, came, *at):
    return add_up([keep[at]] + [v[at[i:]] for i, v in enumerate(came)])


def first_stages(keep, send, stages):
    came = [exchange(send, *stages[0])]
    came.append(exchange(part_of(keep, came, 1).astype(jnp.bfloat16), *stages[1]))
    came.append(exchange(part_of(keep, came, 0, 1).astype(jnp.bfloat16), *stages[2]))
    return (keep, *came)


def join_kernel(*refs):
    halves, outs = (refs[:4], refs[4:8]), refs[8:]
    half = refs[0].shape[-1]
    for n, (keep, *came) in enumerate(halves):
        for m, out in enumerate(outs):
            total = part_of(keep, came, 0, 0, m)
            out[:, n * half : (n + 1) * half] = total.astype(out.dtype)


def join(first, second):
    _, _, last, tall, half = first[0].shape
    vmem = pl.BlockSpec(memory_space=pltpu.VMEM)
    kinds = [jnp.float32] + [jnp.bfloat16] * (last - 1)
    return pl.pallas_call(
        join_kernel,
        out_shape=[pltpu.VMEM((tall, 2 * half), kind) for kind in kinds],
        in_specs=[vmem] * 8,
        out_specs=[vmem] * last,
        compiler_params=pltpu.CompilerParams(vmem_limit_bytes=4 * 2**20),
        name="join",
    )(*in_vmem(*first, *second))


def finish_kernel(*refs):
    terms, (updates, slots) = refs[:-2], refs[-2:]
    total = add_up([v[...] for v in terms]).astype(jnp.bfloat16)
    steps_count, share, cols = updates.shape
    for t in range(steps_count):
        updates[t] = total[t * share : (t + 1) * share]
    slot = total[steps_count * share :]
    for r in range(slot.shape[0]):
        slots[0:1, r * cols : (r + 1) * cols] = slot[r : r + 1]


def finish(steps_count, terms):
    tall, cols = terms[0].shape
    replicas = lax.axis_size("replica")
    share = (tall - replicas) // steps_count
    vmem = pl.BlockSpec(memory_space=pltpu.VMEM)
    return pl.pallas_call(
        finish_kernel,
        out_shape=(
            jax.ShapeDtypeStruct((steps_count, share, cols), jnp.bfloat16),
            jax.ShapeDtypeStruct((1, replicas * cols), jnp.bfloat16),
        ),
        in_specs=[vmem] * len(terms),
        out_specs=(vmem, vmem),
        compiler_params=pltpu.CompilerParams(vmem_limit_bytes=4 * 2**20),
        name="finish",
    )(*in_vmem(*terms))


def move_sums(
    base_stream,
    out_weight,
    queries,
    cache_keys,
    cache_values,
    new_keys,
    new_values,
    lengths,
    finished,
    owners,
):
    steps_count, row_count, heads_here, head_size = queries.shape
    model = out_weight.shape[2]
    split = attend_split(queries, cache_keys, cache_values, new_keys, new_values, lengths)
    gathered = lax.all_to_all(split, "replica", split_axis=0, concat_axis=0, tiled=True)
    gathered = gathered.reshape(-1, gathered.shape[2])
    weight = pltpu.with_memory_space_constraint(out_weight.reshape(-1, model), pltpu.HBM)
    rows, base_rows, early, late = select_rows(owners, finished, weight, steps_count, row_count)
    operands = (gathered, rows, base_rows, base_stream)
    core, across = ("tensor", 1), ("tensor", 2)
    beside, along = ("replica", 1), ("replica", 2)
    second = first_stages(*project(1, *operands, early, weight), (core, beside, across))
    first = first_stages(*project(0, *operands, late, weight), (core, across, beside))
    own, *sends = join(first, second)
    came = [exchange(v, along[0], along[1] * (m + 1)) for m, v in enumerate(sends)]
    updates, trainer_rows = finish(steps_count, (own, *came))
    return (updates, trainer_rows.reshape(1, SLOT_DEV, model))


def shards(*arrays):
    out_weight, queries, cache_keys = arrays[1:4]
    steps_count, row_count, heads_here, head_size = queries.shape
    replicas, tensors = lax.axis_size("replica"), lax.axis_size("tensor")
    sent = steps_count * row_count * replicas
    few = sent <= heads_here * out_weight.shape[1]
    group = heads_here // cache_keys.shape[1]
    shares = replicas * row_count // tensors
    powers = all(n & (n - 1) == 0 for n in (replicas, steps_count, row_count, shares))
    fits = tensors == 4 and replicas == group == 8 and powers and head_size == LANES
    return (move_sums if few and fits else regroup_weight)(*arrays)


def solution(mesh):
    placed = (
        P("tensor", "replica"),
        P("tensor", "replica", None),
        P(None, "replica", "tensor", None),
        P("replica", "tensor", None, None),
        P("replica", "tensor", None, None),
        P(None, "replica", "tensor", None),
        P(None, "replica", "tensor", None),
        P("replica"),
        P(),
        P(),
    )
    return jax.shard_map(
        shards,
        mesh=mesh,
        in_specs=placed,
        out_specs=(P(None, "tensor", "replica"), P("replica", "tensor", None)),
        check_vma=False,
    )
```

```python
import functools
import math

import jax
import jax.numpy as jnp
from jax import lax
from jax.experimental import pallas as pl
from jax.experimental.pallas import tpu as pltpu
from jax.sharding import PartitionSpec as P


SLOT_DEV = 1
LANES = 128
EARLY = (8, 5)


def attend(queries, cache_keys, cache_values, new_keys, new_values, lengths):
    steps_count, row_count, heads_here, head_size = queries.shape
    kv_here = cache_keys.shape[1]
    positions_count = cache_keys.shape[2]
    group_size = heads_here // kv_here
    score_scale = 1.0 / math.sqrt(head_size)
    grouped = queries.reshape(steps_count, row_count, kv_here, group_size, head_size)
    cache_scores = (
        jnp.einsum("tbgqd,bgcd->tbgqc", grouped, cache_keys, preferred_element_type=jnp.float32)
        * score_scale
    )
    positions = lax.broadcasted_iota(jnp.int32, (1, row_count, 1, 1, positions_count), 4)
    is_valid = positions < lengths[None, :, None, None, None]
    cache_scores = jnp.where(is_valid, cache_scores, jnp.float32(-1e30))
    fresh_scores = (
        jnp.einsum("tbgqd,ubgd->tbgqu", grouped, new_keys, preferred_element_type=jnp.float32)
        * score_scale
    )
    step_now = lax.broadcasted_iota(jnp.int32, (steps_count, 1, 1, 1, steps_count), 0)
    step_then = lax.broadcasted_iota(jnp.int32, (steps_count, 1, 1, 1, steps_count), 4)
    fresh_scores = jnp.where(step_then <= step_now, fresh_scores, jnp.float32(-1e30))
    highest = jnp.maximum(
        jnp.max(cache_scores, axis=-1, keepdims=True), jnp.max(fresh_scores, axis=-1, keepdims=True)
    )
    cache_weights = jnp.exp(cache_scores - highest)
    fresh_weights = jnp.exp(fresh_scores - highest)
    totals = jnp.sum(cache_weights, axis=-1, keepdims=True) + jnp.sum(
        fresh_weights, axis=-1, keepdims=True
    )
    cache_probs = (cache_weights / totals).astype(jnp.bfloat16)
    fresh_probs = (fresh_weights / totals).astype(jnp.bfloat16)
    mixed = jnp.einsum(
        "tbgqc,bgcd->tbgqd", cache_probs, cache_values, preferred_element_type=jnp.float32
    )
    mixed = mixed + jnp.einsum(
        "tbgqu,ubgd->tbgqd", fresh_probs, new_values, preferred_element_type=jnp.float32
    )
    return mixed.reshape(steps_count, row_count, heads_here * head_size).astype(jnp.bfloat16)


def reduce_heads(partial_value):
    rounded = partial_value.astype(jnp.bfloat16)
    totals = lax.psum(rounded, "tensor").astype(jnp.float32)
    share = totals.shape[1] // lax.axis_size("tensor")
    return lax.dynamic_slice_in_dim(totals, lax.axis_index("tensor") * share, share, 1)


def regroup_weight(
    base_stream,
    out_weight,
    queries,
    cache_keys,
    cache_values,
    new_keys,
    new_values,
    lengths,
    finished,
    owners,
):
    heads_here = out_weight.shape[0]
    regrouped = lax.all_to_all(out_weight, "replica", split_axis=2, concat_axis=1, tiled=True)
    weight_local = regrouped.reshape(heads_here * regrouped.shape[1], regrouped.shape[2])
    attended = attend(queries, cache_keys, cache_values, new_keys, new_values, lengths)
    partial_value = jnp.einsum(
        "tbf,fc->tbc",
        lax.all_gather(attended, "replica", axis=1, tiled=True),
        weight_local,
        preferred_element_type=jnp.float32,
    )
    summed = reduce_heads(partial_value)
    updates = summed.astype(jnp.bfloat16)
    stream = base_stream.astype(jnp.float32) + jnp.sum(updates.astype(jnp.float32), axis=0)
    stream_rounded = stream.astype(jnp.bfloat16)
    all_streams = lax.all_gather(stream_rounded, "tensor", axis=0, tiled=True)
    owner_count = lax.axis_size("replica")
    owner_ids = lax.broadcasted_iota(jnp.int32, (1, owner_count), 1)
    onehot = (owners == owner_ids).astype(jnp.int32)
    before = jnp.cumsum(onehot, axis=0) - onehot
    slot_rank = jnp.sum(before * onehot, axis=1)
    first_slot = lax.axis_index("tensor") * SLOT_DEV
    slot_ids = first_slot + lax.broadcasted_iota(jnp.int32, (1, 1, SLOT_DEV), 2)
    chosen = (
        onehot[:, :, None]
        * (slot_rank[:, None, None] == slot_ids).astype(jnp.int32)
        * finished[:, None, None]
    )
    selector = chosen.astype(jnp.bfloat16)
    outgoing = jnp.einsum(
        "jos,jc->osc", selector, all_streams, preferred_element_type=jnp.float32
    ).astype(jnp.bfloat16)
    trainer_rows = lax.all_to_all(outgoing, "replica", split_axis=0, concat_axis=2, tiled=True)
    return (updates, trainer_rows)


def attend_kernel(factor, *refs):
    sources, out, places, (fresh_k, fresh_v, turned, sems) = refs[:6], refs[6], refs[7:13], refs[13:]
    lengths, queries, new_keys, new_values, keys, held = places
    steps_count, row_count, heads_here, head_size = queries.shape
    kv_here, positions_count = keys.shape[1], keys.shape[2]
    group = heads_here // kv_here
    lines = steps_count * group
    f32 = jnp.float32
    small = [pltpu.make_async_copy(sources[n], places[n], sems.at[n]) for n in range(4)]
    fetch = lambda n, i: pltpu.make_async_copy(
        sources[4 + n].at[i], places[4 + n].at[i], sems.at[4 + n * row_count + i]
    )
    fetches = [(fetch(0, i), fetch(1, i)) for i in range(row_count)]
    fetches[0][0].start()
    for copy in small:
        copy.start()
    fetches[0][1].start()
    for pair in fetches[1:]:
        pair[0].start()
        pair[1].start()
    fresh_k[...] = jnp.zeros_like(fresh_k)
    fresh_v[...] = jnp.zeros_like(fresh_v)
    place = lax.broadcasted_iota(jnp.int32, (lines, positions_count), 1)
    fresh_at = lax.broadcasted_iota(jnp.int32, (lines, LANES), 1)
    fresh_step = lax.broadcasted_iota(jnp.int32, (lines, LANES), 0) // group
    fresh_valid = fresh_at <= fresh_step
    low = f32(-1e30)
    width = head_size // group
    lane = lax.broadcasted_iota(jnp.int32, (group, head_size), 1) // width
    diagonal = (lane - lax.broadcasted_iota(jnp.int32, (group, head_size), 0)) & (group - 1)
    turn = (((1,), (1,)), ((), ()))

    def fresh_parts(i):
        for g in range(kv_here):
            for t in range(steps_count):
                fresh_k[i, g, t : t + 1] = new_keys[t, i, g : g + 1]
                fresh_v[i, g, t : t + 1] = new_values[t, i, g : g + 1]

    def score(i):
        is_valid = place < lengths[i]
        found = []
        for g in range(kv_here):
            query = jnp.concatenate(
                [queries[t, i, g * group : (g + 1) * group] for t in range(steps_count)], axis=0
            )
            scores = lax.dot_general(query, keys[i, g], turn, preferred_element_type=f32)
            fresh = lax.dot_general(query, fresh_k[i, g], turn, preferred_element_type=f32)
            found.append((jnp.where(is_valid, scores, low), jnp.where(fresh_valid, fresh, low)))
        return found

    def weigh(found):
        weighed = []
        for scores, fresh in found:
            highest = jnp.maximum(
                jnp.max(scores, axis=1, keepdims=True), jnp.max(fresh, axis=1, keepdims=True)
            )
            scores = jnp.exp2((scores - highest) * factor)
            fresh = jnp.exp2((fresh - highest) * factor)
            total = jnp.sum(scores, axis=1, keepdims=True) + jnp.sum(fresh, axis=1, keepdims=True)
            weighed.append((scores.astype(jnp.bfloat16), fresh.astype(jnp.bfloat16), 1.0 / total))
        return weighed

    def mix(i, weighed):
        for g in range(kv_here):
            weights, fresh_weights, share = weighed[g]
            mixed = jnp.dot(weights, held[i, g], preferred_element_type=f32)
            mixed = mixed + jnp.dot(fresh_weights, fresh_v[i, g], preferred_element_type=f32)
            mixed = mixed * share
            for t in range(steps_count):
                part = mixed[t * group : (t + 1) * group]
                moved = jnp.where(diagonal == 0, part, 0.0)
                for d in range(1, group):
                    rolled = pltpu.roll(pltpu.roll(part, group - d, 0), d * width, 1)
                    moved = jnp.where(diagonal == d, rolled, moved)
                turned[g, pl.ds(t * row_count + i, group, stride=steps_count * row_count), :] = moved

    for copy in small:
        copy.wait()
    for i in range(row_count):
        fresh_parts(i)
    fetches[0][0].wait()
    found = score(0)
    for i in range(row_count):
        later = None
        if i + 1 < row_count:
            fetches[i][1].wait()
            fetches[i + 1][0].wait()
            later = score(i + 1)
        else:
            fetches[i][1].wait()
        mix(i, weigh(found))
        found = later
    for g in range(kv_here):
        out[:, :, g * head_size : (g + 1) * head_size] = (
            turned[g].reshape(out.shape[:2] + (head_size,)).astype(jnp.bfloat16)
        )


def in_vmem(*arrays):
    return [pltpu.with_memory_space_constraint(v, pltpu.VMEM) for v in arrays]


def in_hbm(*arrays):
    return [pltpu.with_memory_space_constraint(v, pltpu.HBM) for v in arrays]


def attend_split(queries, cache_keys, cache_values, new_keys, new_values, lengths):
    steps_count, row_count, heads_here, head_size = queries.shape
    _, kv_here, positions_count, _ = cache_keys.shape
    group = heads_here // kv_here
    lines = steps_count * row_count
    operands = (lengths, queries, new_keys, new_values, cache_keys, cache_values)
    vmem = pl.BlockSpec(memory_space=pltpu.VMEM)
    (out,) = pl.pallas_call(
        functools.partial(attend_kernel, math.log2(math.e) / math.sqrt(head_size)),
        out_shape=(pltpu.VMEM((group, lines, kv_here * head_size), jnp.bfloat16),),
        in_specs=[pl.BlockSpec(memory_space=pltpu.HBM)] * len(operands),
        out_specs=(vmem,),
        scratch_shapes=[
            pltpu.SMEM(lengths.shape, lengths.dtype),
            *(pltpu.VMEM(v.shape, v.dtype) for v in operands[1:]),
            pltpu.VMEM((row_count, kv_here, LANES, head_size), jnp.bfloat16),
            pltpu.VMEM((row_count, kv_here, LANES, head_size), jnp.bfloat16),
            pltpu.VMEM((kv_here, group * lines, head_size), jnp.float32),
            pltpu.SemaphoreType.DMA((4 + 2 * row_count,)),
        ],
        compiler_params=pltpu.CompilerParams(vmem_limit_bytes=16 * 2**20),
        cost_estimate=pl.CostEstimate(
            flops=4 * lines * heads_here * positions_count * head_size,
            bytes_accessed=4 * row_count * kv_here * positions_count * head_size,
            transcendentals=lines * heads_here * positions_count,
        ),
        name="attend",
    )(*in_hbm(*operands))
    return out


def fetch_weight(weight, held, sems, columns, blocks):
    start, width = columns
    block = weight.shape[1] // lax.axis_size("replica")
    me = lax.axis_index("replica")
    return [
        pltpu.make_async_copy(
            weight.at[:, pl.ds(pl.multiple_of((r ^ me) * block + start, LANES), width)],
            held.at[:, pl.ds(n * width, width)],
            sems.at[n],
        )
        for n, r in enumerate(blocks)
    ]


def select_kernel(sizes, calls, owners_at, finished_at, weight, rows, base_rows, *refs):
    tensors, replicas, steps_count, row_count = sizes
    held, (owners, finished, small), sems = refs[: len(calls)], refs[len(calls) :][:3], refs[len(calls) + 3 :]
    total_rows = replicas * row_count
    share = total_rows // tensors
    lines = steps_count * share
    me_r, me_t = lax.axis_index("replica"), lax.axis_index("tensor")
    first = [
        pltpu.make_async_copy(owners_at, owners, small.at[0]),
        pltpu.make_async_copy(finished_at, finished, small.at[1]),
    ]
    fetches = []
    for columns, ref, sem in zip(calls, held, sems):
        fetches += fetch_weight(weight, ref, sem, columns, range(ref.shape[1] // columns[1]))
    for fetch in first + fetches:
        fetch.start()
    for fetch in first:
        fetch.wait()

    def tell(row_of):
        name, rank, done = (jnp.zeros_like(row_of) for _ in range(3))
        for j in range(total_rows):
            name = jnp.where(row_of == j, owners[j], name)
            done = jnp.where(row_of == j, finished[j], done)
        for j in range(total_rows):
            rank = rank + jnp.where((name == owners[j]) & (row_of > j), 1, 0)
        return jnp.where(done > 0, name, -1), rank

    width = steps_count * total_rows
    col = lax.broadcasted_iota(jnp.int32, (1, width), 1)
    per = steps_count * row_count
    row_of = col // per * row_count + (col & (row_count - 1))
    step_of = (col & (per - 1)) // row_count
    name, rank = tell(row_of)
    own = lax.broadcasted_iota(jnp.int32, (1, LANES), 1)
    base_name, base_rank = tell(own + me_t * share)
    base_name = jnp.where(own < share, base_name, -1)
    line = lax.broadcasted_iota(jnp.int32, (lines, width), 0)
    line_row, line_step = line & (share - 1), line // share
    owner = lax.broadcasted_iota(jnp.int32, (replicas, width), 0) ^ me_r
    base_owner = lax.broadcasted_iota(jnp.int32, (replicas, LANES), 0) ^ me_r
    picked = lambda hit: jnp.where(hit, 1.0, 0.0).astype(jnp.bfloat16)
    for t in range(tensors):
        target = me_t ^ t
        hit = (row_of == target * share + line_row) & (step_of == line_step)
        first = t * (lines + replicas)
        rows[first : first + lines] = picked(hit)
        hit = (name == owner) & (rank == target)
        rows[first + lines : first + lines + replicas] = picked(hit)
        hit = (base_name == base_owner) & (base_rank == target)
        base_rows[t * replicas : (t + 1) * replicas] = picked(hit)[:, :share]
    for fetch in fetches:
        fetch.wait()


def select_rows(owners, finished, weight, calls, early, steps_count, row_count):
    replicas, tensors = lax.axis_size("replica"), lax.axis_size("tensor")
    share = replicas * row_count // tensors
    hbm, vmem = pl.BlockSpec(memory_space=pltpu.HBM), pl.BlockSpec(memory_space=pltpu.VMEM)
    height = tensors * (steps_count * share + replicas)
    names = owners[:, 0]
    return pl.pallas_call(
        functools.partial(select_kernel, (tensors, replicas, steps_count, row_count), calls),
        out_shape=(
            pltpu.VMEM((height, steps_count * replicas * row_count), jnp.bfloat16),
            pltpu.VMEM((tensors * replicas, share), jnp.bfloat16),
            *(
                pltpu.VMEM((weight.shape[0], blocks * width), weight.dtype)
                for blocks, (_, width) in zip(early, calls)
            ),
        ),
        in_specs=[hbm] * 3,
        out_specs=[vmem] * (2 + len(calls)),
        scratch_shapes=[
            pltpu.SMEM(names.shape, names.dtype),
            pltpu.SMEM(finished.shape, finished.dtype),
            pltpu.SemaphoreType.DMA((2,)),
            *(pltpu.SemaphoreType.DMA((blocks,)) for blocks in early),
        ],
        compiler_params=pltpu.CompilerParams(vmem_limit_bytes=4 * 2**20),
        cost_estimate=pl.CostEstimate(
            flops=10**6, bytes_accessed=2 * weight.size, transcendentals=0
        ),
        name="select",
    )(*in_hbm(names, finished, weight))


def place(order, t, r):
    tensors, replicas = lax.axis_size("tensor"), lax.axis_size("replica")
    bits = {"x": (t // 2, tensors // 2), "y": (r % 2, 2), "z": (r // 2, replicas // 2)}
    at = 0
    for name in order:
        at = at * bits[name][1] + bits[name][0]
    return at


def project_kernel(sizes, columns, order, later, *refs):
    gathered, rows, base_rows, base, near, rest = refs[:6]
    tensors, replicas, lines = sizes
    fetches = []
    if later is None:
        keep, send, slot_sums = refs[6:]
    else:
        keep, send, fetched, slot_sums, sems = refs[6:]
        fetches = fetch_weight(rest, fetched, sems, later[0], range(later[1], replicas))
    start, width = columns
    f32 = jnp.float32
    me = lax.axis_index("replica")
    tall = lines + replicas
    found = near.shape[1] // width
    for fetch in fetches:
        fetch.start()
    held = jnp.dot(rows[...], gathered[...], preferred_element_type=f32).astype(jnp.bfloat16)
    extra = jnp.dot(
        base_rows[...], base[:, start : start + width], preferred_element_type=f32
    )

    def target(t, r):
        return (send if t % 2 else keep).at[place(order, t, r)]

    for r in range(replicas):
        block = r ^ me
        if r < found:
            own = near[:, r * width : (r + 1) * width]
        else:
            own = rest[:, (r - found) * width : (r - found + 1) * width]
        sums = jnp.dot(held, own, preferred_element_type=f32)
        for t in range(tensors):
            top = t * tall
            target(t, r)[:lines] = sums[top : top + lines].astype(jnp.bfloat16)
            slot = sums[top + lines : top + tall]
            if r == 0:
                slot = slot + extra[t * replicas : (t + 1) * replicas]
            for c in range(width // LANES):
                slot_sums[t, c, pl.ds(block, replicas, stride=replicas), :] = slot[
                    :, c * LANES : (c + 1) * LANES
                ]
    for t in range(tensors):
        for r in range(replicas):
            for c in range(width // LANES):
                target(t, r)[lines:, c * LANES : (c + 1) * LANES] = slot_sums[
                    t, c, r * replicas : (r + 1) * replicas
                ].astype(jnp.bfloat16)
    for fetch in fetches:
        fetch.wait()


def project(columns, order, later, gathered, rows, base_rows, base_stream, near, rest):
    replicas, tensors = lax.axis_size("replica"), lax.axis_size("tensor")
    depth = near.shape[0]
    width = columns[1]
    tall = rows.shape[0] // tensors
    shape = pltpu.VMEM((tensors // 2 * replicas, tall, width), jnp.bfloat16)
    vmem = pl.BlockSpec(memory_space=pltpu.VMEM)
    slot_sums = pltpu.VMEM((tensors, width // LANES, replicas * replicas, LANES), jnp.float32)
    fetched, sems, space, constrain = (), (), pltpu.VMEM, in_vmem
    if later is not None:
        missing = replicas - later[1]
        fetched = (pltpu.VMEM((depth, missing * later[0][1]), near.dtype),)
        sems = (pltpu.SemaphoreType.DMA((missing,)),)
        space, constrain = pltpu.HBM, in_hbm
    return pl.pallas_call(
        functools.partial(
            project_kernel, (tensors, replicas, tall - replicas), columns, order, later
        ),
        out_shape=(shape, shape, *fetched),
        in_specs=[vmem] * 5 + [pl.BlockSpec(memory_space=space)],
        out_specs=(vmem,) * (2 + len(fetched)),
        scratch_shapes=[slot_sums, *sems],
        compiler_params=pltpu.CompilerParams(vmem_limit_bytes=8 * 2**20),
        cost_estimate=pl.CostEstimate(
            flops=2 * rows.shape[0] * depth * width * replicas,
            bytes_accessed=2 * depth * width * replicas,
            transcendentals=0,
        ),
    )(*in_vmem(gathered, rows, base_rows, base_stream, near), *constrain(rest))


def exchange(value, axis, mask):
    size = lax.axis_size(axis)
    return lax.ppermute(value, axis, [(i, i ^ mask) for i in range(size)])


def add_up(terms):
    return functools.reduce(jnp.add, [v.astype(jnp.float32) for v in terms])


def halve(kept, axis, mask):
    half = kept[-1].shape[0] // 2
    part = add_up([v[half : 2 * half] for v in kept]).astype(jnp.bfloat16)
    return kept + [exchange(part, axis, mask)]


def join_kernel(count, *refs):
    groups, outs = (refs[:count], refs[count : 2 * count]), refs[2 * count :]
    for n, group in enumerate(groups):
        for m, out in enumerate(outs):
            total = add_up([v[m] for v in group])
            width = total.shape[1]
            out[:, n * width : (n + 1) * width] = total.astype(out.dtype)


def join(first, second, last):
    _, tall, width = first[-1].shape
    vmem = pl.BlockSpec(memory_space=pltpu.VMEM)
    kinds = [jnp.float32] + [jnp.bfloat16] * (last - 1)
    return pl.pallas_call(
        functools.partial(join_kernel, len(first)),
        out_shape=[pltpu.VMEM((tall, 2 * width), kind) for kind in kinds],
        in_specs=[vmem] * (2 * len(first)),
        out_specs=[vmem] * last,
        compiler_params=pltpu.CompilerParams(vmem_limit_bytes=4 * 2**20),
        name="join",
    )(*in_vmem(*first, *second))


def finish_kernel(*refs):
    terms, (updates, slots) = refs[:-2], refs[-2:]
    total = add_up([v[...] for v in terms]).astype(jnp.bfloat16)
    steps_count, share, cols = updates.shape
    for t in range(steps_count):
        updates[t] = total[t * share : (t + 1) * share]
    slot = total[steps_count * share :]
    for r in range(slot.shape[0]):
        slots[0:1, r * cols : (r + 1) * cols] = slot[r : r + 1]


def finish(steps_count, terms):
    tall, cols = terms[0].shape
    replicas = lax.axis_size("replica")
    share = (tall - replicas) // steps_count
    vmem = pl.BlockSpec(memory_space=pltpu.VMEM)
    return pl.pallas_call(
        finish_kernel,
        out_shape=(
            jax.ShapeDtypeStruct((steps_count, share, cols), jnp.bfloat16),
            jax.ShapeDtypeStruct((1, replicas * cols), jnp.bfloat16),
        ),
        in_specs=[vmem] * len(terms),
        out_specs=(vmem, vmem),
        compiler_params=pltpu.CompilerParams(vmem_limit_bytes=4 * 2**20),
        name="finish",
    )(*in_vmem(*terms))


def move_sums(
    base_stream,
    out_weight,
    queries,
    cache_keys,
    cache_values,
    new_keys,
    new_values,
    lengths,
    finished,
    owners,
):
    steps_count, row_count, _, _ = queries.shape
    replicas = lax.axis_size("replica")
    model = out_weight.shape[2]
    split = attend_split(queries, cache_keys, cache_values, new_keys, new_values, lengths)
    gathered = lax.all_to_all(split, "replica", split_axis=0, concat_axis=0, tiled=True)
    gathered = gathered.reshape(-1, gathered.shape[2])
    weight = out_weight.reshape(-1, model)
    cols = model // replicas
    half = cols // 2
    calls = ((0, half), (half, half))
    rows, base_rows, *near = select_rows(
        owners, finished, weight, calls, EARLY, steps_count, row_count
    )
    operands = (gathered, rows, base_rows, base_stream)
    core, across = ("tensor", 1), ("tensor", 2)
    beside, along = ("replica", 1), ("replica", 2)
    later = (calls[1], EARLY[1])
    keep, send, rest = project(calls[0], "xyz", later, *operands, near[0], weight)
    first = [keep, exchange(send, *core)]
    keep, send = project(calls[1], "yxz", None, *operands, near[1], rest)
    second = [keep, exchange(send, *core)]
    first = halve(first, *across)
    first = halve(first, *beside)
    second = halve(second, *beside)
    second = halve(second, *across)
    own, *sends = join(first, second, replicas // 2)
    came = [exchange(v, along[0], along[1] * (m + 1)) for m, v in enumerate(sends)]
    updates, trainer_rows = finish(steps_count, (own, *came))
    return (updates, trainer_rows.reshape(1, SLOT_DEV, model))


def shards(*arrays):
    out_weight, queries, cache_keys = arrays[1:4]
    steps_count, row_count, heads_here, head_size = queries.shape
    replicas, tensors = lax.axis_size("replica"), lax.axis_size("tensor")
    sent = steps_count * row_count * replicas
    few = sent <= heads_here * out_weight.shape[1]
    group = heads_here // cache_keys.shape[1]
    shares = replicas * row_count // tensors
    powers = all(n & (n - 1) == 0 for n in (replicas, steps_count, row_count, shares))
    fits = tensors == 4 and replicas == group == 8 and powers and head_size == LANES
    fits = fits and out_weight.shape[2] % (replicas * 2 * LANES) == 0
    if not (few and fits):
        return regroup_weight(*arrays)
    return move_sums(*arrays)


def solution(mesh):
    placed = (
        P("tensor", "replica"),
        P("tensor", "replica", None),
        P(None, "replica", "tensor", None),
        P("replica", "tensor", None, None),
        P("replica", "tensor", None, None),
        P(None, "replica", "tensor", None),
        P(None, "replica", "tensor", None),
        P("replica"),
        P(),
        P(),
    )
    return jax.shard_map(
        shards,
        mesh=mesh,
        in_specs=placed,
        out_specs=(P(None, "tensor", "replica"), P("replica", "tensor", None)),
        check_vma=False,
    )
```

```python
import functools
import math

import jax
import jax.numpy as jnp
from jax import lax
from jax.experimental import pallas as pl
from jax.experimental.pallas import tpu as pltpu
from jax.sharding import PartitionSpec as P


SLOT_DEV = 1
LANES = 128
EARLY = (8, 5)


def attend(queries, cache_keys, cache_values, new_keys, new_values, lengths):
    steps_count, row_count, heads_here, head_size = queries.shape
    kv_here = cache_keys.shape[1]
    positions_count = cache_keys.shape[2]
    group_size = heads_here // kv_here
    score_scale = 1.0 / math.sqrt(head_size)
    grouped = queries.reshape(steps_count, row_count, kv_here, group_size, head_size)
    cache_scores = (
        jnp.einsum("tbgqd,bgcd->tbgqc", grouped, cache_keys, preferred_element_type=jnp.float32)
        * score_scale
    )
    positions = lax.broadcasted_iota(jnp.int32, (1, row_count, 1, 1, positions_count), 4)
    is_valid = positions < lengths[None, :, None, None, None]
    cache_scores = jnp.where(is_valid, cache_scores, jnp.float32(-1e30))
    fresh_scores = (
        jnp.einsum("tbgqd,ubgd->tbgqu", grouped, new_keys, preferred_element_type=jnp.float32)
        * score_scale
    )
    step_now = lax.broadcasted_iota(jnp.int32, (steps_count, 1, 1, 1, steps_count), 0)
    step_then = lax.broadcasted_iota(jnp.int32, (steps_count, 1, 1, 1, steps_count), 4)
    fresh_scores = jnp.where(step_then <= step_now, fresh_scores, jnp.float32(-1e30))
    highest = jnp.maximum(
        jnp.max(cache_scores, axis=-1, keepdims=True), jnp.max(fresh_scores, axis=-1, keepdims=True)
    )
    cache_weights = jnp.exp(cache_scores - highest)
    fresh_weights = jnp.exp(fresh_scores - highest)
    totals = jnp.sum(cache_weights, axis=-1, keepdims=True) + jnp.sum(
        fresh_weights, axis=-1, keepdims=True
    )
    cache_probs = (cache_weights / totals).astype(jnp.bfloat16)
    fresh_probs = (fresh_weights / totals).astype(jnp.bfloat16)
    mixed = jnp.einsum(
        "tbgqc,bgcd->tbgqd", cache_probs, cache_values, preferred_element_type=jnp.float32
    )
    mixed = mixed + jnp.einsum(
        "tbgqu,ubgd->tbgqd", fresh_probs, new_values, preferred_element_type=jnp.float32
    )
    return mixed.reshape(steps_count, row_count, heads_here * head_size).astype(jnp.bfloat16)


def reduce_heads(partial_value):
    rounded = partial_value.astype(jnp.bfloat16)
    totals = lax.psum(rounded, "tensor").astype(jnp.float32)
    share = totals.shape[1] // lax.axis_size("tensor")
    return lax.dynamic_slice_in_dim(totals, lax.axis_index("tensor") * share, share, 1)


def regroup_weight(
    base_stream,
    out_weight,
    queries,
    cache_keys,
    cache_values,
    new_keys,
    new_values,
    lengths,
    finished,
    owners,
):
    heads_here = out_weight.shape[0]
    regrouped = lax.all_to_all(out_weight, "replica", split_axis=2, concat_axis=1, tiled=True)
    weight_local = regrouped.reshape(heads_here * regrouped.shape[1], regrouped.shape[2])
    attended = attend(queries, cache_keys, cache_values, new_keys, new_values, lengths)
    partial_value = jnp.einsum(
        "tbf,fc->tbc",
        lax.all_gather(attended, "replica", axis=1, tiled=True),
        weight_local,
        preferred_element_type=jnp.float32,
    )
    summed = reduce_heads(partial_value)
    updates = summed.astype(jnp.bfloat16)
    stream = base_stream.astype(jnp.float32) + jnp.sum(updates.astype(jnp.float32), axis=0)
    stream_rounded = stream.astype(jnp.bfloat16)
    all_streams = lax.all_gather(stream_rounded, "tensor", axis=0, tiled=True)
    owner_count = lax.axis_size("replica")
    owner_ids = lax.broadcasted_iota(jnp.int32, (1, owner_count), 1)
    onehot = (owners == owner_ids).astype(jnp.int32)
    before = jnp.cumsum(onehot, axis=0) - onehot
    slot_rank = jnp.sum(before * onehot, axis=1)
    first_slot = lax.axis_index("tensor") * SLOT_DEV
    slot_ids = first_slot + lax.broadcasted_iota(jnp.int32, (1, 1, SLOT_DEV), 2)
    chosen = (
        onehot[:, :, None]
        * (slot_rank[:, None, None] == slot_ids).astype(jnp.int32)
        * finished[:, None, None]
    )
    selector = chosen.astype(jnp.bfloat16)
    outgoing = jnp.einsum(
        "jos,jc->osc", selector, all_streams, preferred_element_type=jnp.float32
    ).astype(jnp.bfloat16)
    trainer_rows = lax.all_to_all(outgoing, "replica", split_axis=0, concat_axis=2, tiled=True)
    return (updates, trainer_rows)


def attend_kernel(factor, *refs):
    sources, out, places, (fresh_k, fresh_v, turned, sems) = refs[:6], refs[6], refs[7:13], refs[13:]
    lengths, queries, new_keys, new_values, keys, held = places
    steps_count, row_count, heads_here, head_size = queries.shape
    kv_here, positions_count = keys.shape[1], keys.shape[2]
    group = heads_here // kv_here
    lines = steps_count * group
    f32 = jnp.float32
    small = [pltpu.make_async_copy(sources[n], places[n], sems.at[n]) for n in range(4)]
    fetch = lambda n, i: pltpu.make_async_copy(
        sources[4 + n].at[i], places[4 + n].at[i], sems.at[4 + n * row_count + i]
    )
    fetches = [(fetch(0, i), fetch(1, i)) for i in range(row_count)]
    fetches[0][0].start()
    for copy in small:
        copy.start()
    for i in range(1, row_count + 1):
        if i < row_count:
            fetches[i][0].start()
        fetches[i - 1][1].start()
    fresh_k[...] = jnp.zeros_like(fresh_k)
    fresh_v[...] = jnp.zeros_like(fresh_v)
    place = lax.broadcasted_iota(jnp.int32, (lines, positions_count), 1)
    fresh_at = lax.broadcasted_iota(jnp.int32, (lines, LANES), 1)
    fresh_step = lax.broadcasted_iota(jnp.int32, (lines, LANES), 0) // group
    fresh_valid = fresh_at <= fresh_step
    low = f32(-1e30)
    width = head_size // group
    lane = lax.broadcasted_iota(jnp.int32, (group, head_size), 1) // width
    diagonal = (lane - lax.broadcasted_iota(jnp.int32, (group, head_size), 0)) & (group - 1)
    turn = (((1,), (1,)), ((), ()))

    def fresh_parts(i):
        for g in range(kv_here):
            for t in range(steps_count):
                fresh_k[i, g, t : t + 1] = new_keys[t, i, g : g + 1]
                fresh_v[i, g, t : t + 1] = new_values[t, i, g : g + 1]

    def score(i):
        is_valid = place < lengths[i]
        found = []
        for g in range(kv_here):
            query = jnp.concatenate(
                [queries[t, i, g * group : (g + 1) * group] for t in range(steps_count)], axis=0
            )
            scores = lax.dot_general(query, keys[i, g], turn, preferred_element_type=f32)
            fresh = lax.dot_general(query, fresh_k[i, g], turn, preferred_element_type=f32)
            found.append((jnp.where(is_valid, scores, low), jnp.where(fresh_valid, fresh, low)))
        return found

    def weigh(found):
        weighed = []
        for scores, fresh in found:
            highest = jnp.maximum(
                jnp.max(scores, axis=1, keepdims=True), jnp.max(fresh, axis=1, keepdims=True)
            )
            scores = jnp.exp2((scores - highest) * factor)
            fresh = jnp.exp2((fresh - highest) * factor)
            total = jnp.sum(scores, axis=1, keepdims=True) + jnp.sum(fresh, axis=1, keepdims=True)
            weighed.append((scores.astype(jnp.bfloat16), fresh.astype(jnp.bfloat16), 1.0 / total))
        return weighed

    def mix(i, weighed):
        for g in range(kv_here):
            weights, fresh_weights, share = weighed[g]
            mixed = jnp.dot(weights, held[i, g], preferred_element_type=f32)
            mixed = mixed + jnp.dot(fresh_weights, fresh_v[i, g], preferred_element_type=f32)
            mixed = mixed * share
            for t in range(steps_count):
                part = mixed[t * group : (t + 1) * group]
                moved = jnp.where(diagonal == 0, part, 0.0)
                for d in range(1, group):
                    rolled = pltpu.roll(pltpu.roll(part, group - d, 0), d * width, 1)
                    moved = jnp.where(diagonal == d, rolled, moved)
                turned[g, pl.ds(t * row_count + i, group, stride=steps_count * row_count), :] = moved

    for copy in small:
        copy.wait()
    for i in range(row_count):
        fresh_parts(i)
    found, weighed = {}, {}
    for i in range(row_count + 2):
        if i < row_count:
            fetches[i][0].wait()
        if i >= 2:
            fetches[i - 2][1].wait()
        if i < row_count:
            found[i] = score(i)
        if 1 <= i <= row_count:
            weighed[i - 1] = weigh(found.pop(i - 1))
        if i >= 2:
            mix(i - 2, weighed.pop(i - 2))
    for g in range(kv_here):
        out[:, :, g * head_size : (g + 1) * head_size] = (
            turned[g].reshape(out.shape[:2] + (head_size,)).astype(jnp.bfloat16)
        )


def in_vmem(*arrays):
    return [pltpu.with_memory_space_constraint(v, pltpu.VMEM) for v in arrays]


def in_hbm(*arrays):
    return [pltpu.with_memory_space_constraint(v, pltpu.HBM) for v in arrays]


def attend_split(queries, cache_keys, cache_values, new_keys, new_values, lengths):
    steps_count, row_count, heads_here, head_size = queries.shape
    _, kv_here, positions_count, _ = cache_keys.shape
    group = heads_here // kv_here
    lines = steps_count * row_count
    operands = (lengths, queries, new_keys, new_values, cache_keys, cache_values)
    vmem = pl.BlockSpec(memory_space=pltpu.VMEM)
    (out,) = pl.pallas_call(
        functools.partial(attend_kernel, math.log2(math.e) / math.sqrt(head_size)),
        out_shape=(pltpu.VMEM((group, lines, kv_here * head_size), jnp.bfloat16),),
        in_specs=[pl.BlockSpec(memory_space=pltpu.HBM)] * len(operands),
        out_specs=(vmem,),
        scratch_shapes=[
            pltpu.SMEM(lengths.shape, lengths.dtype),
            *(pltpu.VMEM(v.shape, v.dtype) for v in operands[1:]),
            pltpu.VMEM((row_count, kv_here, LANES, head_size), jnp.bfloat16),
            pltpu.VMEM((row_count, kv_here, LANES, head_size), jnp.bfloat16),
            pltpu.VMEM((kv_here, group * lines, head_size), jnp.float32),
            pltpu.SemaphoreType.DMA((4 + 2 * row_count,)),
        ],
        compiler_params=pltpu.CompilerParams(vmem_limit_bytes=16 * 2**20),
        cost_estimate=pl.CostEstimate(
            flops=4 * lines * heads_here * positions_count * head_size,
            bytes_accessed=4 * row_count * kv_here * positions_count * head_size,
            transcendentals=lines * heads_here * positions_count,
        ),
        name="attend",
    )(*in_hbm(*operands))
    return out


def fetch_weight(weight, held, sems, columns, blocks):
    start, width = columns
    block = weight.shape[1] // lax.axis_size("replica")
    me = lax.axis_index("replica")
    return [
        pltpu.make_async_copy(
            weight.at[:, pl.ds(pl.multiple_of((r ^ me) * block + start, LANES), width)],
            held.at[:, pl.ds(n * width, width)],
            sems.at[n],
        )
        for n, r in enumerate(blocks)
    ]


def select_kernel(sizes, calls, owners_at, finished_at, weight, rows, base_rows, *refs):
    tensors, replicas, steps_count, row_count = sizes
    held, far = refs[: len(calls)], refs[len(calls)]
    owners, finished, small, bounce, far_sems, *sems = refs[len(calls) + 1 :]
    total_rows = replicas * row_count
    share = total_rows // tensors
    lines = steps_count * share
    me_r, me_t = lax.axis_index("replica"), lax.axis_index("tensor")
    first = [
        pltpu.make_async_copy(owners_at, owners, small.at[0]),
        pltpu.make_async_copy(finished_at, finished, small.at[1]),
    ]
    width = calls[-1][1]
    missing = range(held[-1].shape[1] // width, replicas)
    turns = fetch_weight(weight, bounce, far_sems, calls[-1], missing)
    settle = pltpu.make_async_copy(bounce, far, far_sems.at[len(missing)])
    for fetch in turns:
        fetch.start()
    fetches = []
    for columns, ref, sem in zip(calls, held, sems):
        fetches += fetch_weight(weight, ref, sem, columns, range(ref.shape[1] // columns[1]))
    for fetch in first + fetches:
        fetch.start()
    for fetch in turns:
        fetch.wait()
    settle.start()
    for fetch in first:
        fetch.wait()

    def tell(row_of):
        name, rank, done = (jnp.zeros_like(row_of) for _ in range(3))
        for j in range(total_rows):
            name = jnp.where(row_of == j, owners[j], name)
            done = jnp.where(row_of == j, finished[j], done)
        for j in range(total_rows):
            rank = rank + jnp.where((name == owners[j]) & (row_of > j), 1, 0)
        return jnp.where(done > 0, name, -1), rank

    width = steps_count * total_rows
    col = lax.broadcasted_iota(jnp.int32, (1, width), 1)
    per = steps_count * row_count
    row_of = col // per * row_count + (col & (row_count - 1))
    step_of = (col & (per - 1)) // row_count
    name, rank = tell(row_of)
    own = lax.broadcasted_iota(jnp.int32, (1, LANES), 1)
    base_name, base_rank = tell(own + me_t * share)
    base_name = jnp.where(own < share, base_name, -1)
    line = lax.broadcasted_iota(jnp.int32, (lines, width), 0)
    line_row, line_step = line & (share - 1), line // share
    owner = lax.broadcasted_iota(jnp.int32, (replicas, width), 0) ^ me_r
    base_owner = lax.broadcasted_iota(jnp.int32, (replicas, LANES), 0) ^ me_r
    picked = lambda hit: jnp.where(hit, 1.0, 0.0).astype(jnp.bfloat16)
    for t in range(tensors):
        target = me_t ^ t
        hit = (row_of == target * share + line_row) & (step_of == line_step)
        first = t * (lines + replicas)
        rows[first : first + lines] = picked(hit)
        hit = (name == owner) & (rank == target)
        rows[first + lines : first + lines + replicas] = picked(hit)
        hit = (base_name == base_owner) & (base_rank == target)
        base_rows[t * replicas : (t + 1) * replicas] = picked(hit)[:, :share]
    for fetch in fetches:
        fetch.wait()
    settle.wait()


def select_rows(owners, finished, weight, calls, early, steps_count, row_count):
    replicas, tensors = lax.axis_size("replica"), lax.axis_size("tensor")
    share = replicas * row_count // tensors
    hbm, vmem = pl.BlockSpec(memory_space=pltpu.HBM), pl.BlockSpec(memory_space=pltpu.VMEM)
    height = tensors * (steps_count * share + replicas)
    names = owners[:, 0]
    far = (weight.shape[0], (replicas - early[-1]) * calls[-1][1])
    return pl.pallas_call(
        functools.partial(select_kernel, (tensors, replicas, steps_count, row_count), calls),
        out_shape=(
            pltpu.VMEM((height, steps_count * replicas * row_count), jnp.bfloat16),
            pltpu.VMEM((tensors * replicas, share), jnp.bfloat16),
            *(
                pltpu.VMEM((weight.shape[0], blocks * width), weight.dtype)
                for blocks, (_, width) in zip(early, calls)
            ),
            pltpu.HBM(far, weight.dtype),
        ),
        in_specs=[hbm] * 3,
        out_specs=[vmem] * (2 + len(calls)) + [hbm],
        scratch_shapes=[
            pltpu.SMEM(names.shape, names.dtype),
            pltpu.SMEM(finished.shape, finished.dtype),
            pltpu.SemaphoreType.DMA((2,)),
            pltpu.VMEM(far, weight.dtype),
            pltpu.SemaphoreType.DMA((replicas - early[-1] + 1,)),
            *(pltpu.SemaphoreType.DMA((blocks,)) for blocks in early),
        ],
        compiler_params=pltpu.CompilerParams(vmem_limit_bytes=4 * 2**20),
        cost_estimate=pl.CostEstimate(
            flops=10**6, bytes_accessed=2 * weight.size, transcendentals=0
        ),
        name="select",
    )(*in_hbm(names, finished, weight))


def place(order, t, r):
    tensors, replicas = lax.axis_size("tensor"), lax.axis_size("replica")
    bits = {"x": (t // 2, tensors // 2), "y": (r % 2, 2), "z": (r // 2, replicas // 2)}
    at = 0
    for name in order:
        at = at * bits[name][1] + bits[name][0]
    return at


def project_kernel(sizes, columns, order, *refs):
    gathered, rows, base_rows, base, near, rest, keep, send, slot_sums = refs
    tensors, replicas, lines = sizes
    start, width = columns
    f32 = jnp.float32
    me = lax.axis_index("replica")
    tall = lines + replicas
    found = near.shape[1] // width
    held = jnp.dot(rows[...], gathered[...], preferred_element_type=f32).astype(jnp.bfloat16)
    extra = jnp.dot(
        base_rows[...], base[:, start : start + width], preferred_element_type=f32
    )

    def target(t, r):
        return (send if t % 2 else keep).at[place(order, t, r)]

    for r in range(replicas):
        block = r ^ me
        if r < found:
            own = near[:, r * width : (r + 1) * width]
        else:
            own = rest[:, (r - found) * width : (r - found + 1) * width]
        sums = jnp.dot(held, own, preferred_element_type=f32)
        for t in range(tensors):
            top = t * tall
            target(t, r)[:lines] = sums[top : top + lines].astype(jnp.bfloat16)
            slot = sums[top + lines : top + tall]
            if r == 0:
                slot = slot + extra[t * replicas : (t + 1) * replicas]
            for c in range(width // LANES):
                slot_sums[t, c, pl.ds(block, replicas, stride=replicas), :] = slot[
                    :, c * LANES : (c + 1) * LANES
                ]
    for t in range(tensors):
        for r in range(replicas):
            for c in range(width // LANES):
                target(t, r)[lines:, c * LANES : (c + 1) * LANES] = slot_sums[
                    t, c, r * replicas : (r + 1) * replicas
                ].astype(jnp.bfloat16)


def project(columns, order, gathered, rows, base_rows, base_stream, near, rest):
    replicas, tensors = lax.axis_size("replica"), lax.axis_size("tensor")
    depth = near.shape[0]
    width = columns[1]
    tall = rows.shape[0] // tensors
    shape = pltpu.VMEM((tensors // 2 * replicas, tall, width), jnp.bfloat16)
    vmem = pl.BlockSpec(memory_space=pltpu.VMEM)
    slot_sums = pltpu.VMEM((tensors, width // LANES, replicas * replicas, LANES), jnp.float32)
    return pl.pallas_call(
        functools.partial(
            project_kernel, (tensors, replicas, tall - replicas), columns, order
        ),
        out_shape=(shape, shape),
        in_specs=[vmem] * 6,
        out_specs=(vmem, vmem),
        scratch_shapes=[slot_sums],
        compiler_params=pltpu.CompilerParams(vmem_limit_bytes=8 * 2**20),
        cost_estimate=pl.CostEstimate(
            flops=2 * rows.shape[0] * depth * width * replicas,
            bytes_accessed=2 * depth * width * replicas,
            transcendentals=0,
        ),
    )(*in_vmem(gathered, rows, base_rows, base_stream, near, rest))


def exchange(value, axis, mask):
    size = lax.axis_size(axis)
    return lax.ppermute(value, axis, [(i, i ^ mask) for i in range(size)])


def add_up(terms):
    return functools.reduce(jnp.add, [v.astype(jnp.float32) for v in terms])


def halve(kept, axis, mask):
    half = kept[-1].shape[0] // 2
    part = add_up([v[half : 2 * half] for v in kept]).astype(jnp.bfloat16)
    return kept + [exchange(part, axis, mask)]


def join_kernel(count, *refs):
    groups, outs = (refs[:count], refs[count : 2 * count]), refs[2 * count :]
    for n, group in enumerate(groups):
        for m, out in enumerate(outs):
            total = add_up([v[m] for v in group])
            width = total.shape[1]
            out[:, n * width : (n + 1) * width] = total.astype(out.dtype)


def join(first, second, last):
    _, tall, width = first[-1].shape
    vmem = pl.BlockSpec(memory_space=pltpu.VMEM)
    kinds = [jnp.float32] + [jnp.bfloat16] * (last - 1)
    return pl.pallas_call(
        functools.partial(join_kernel, len(first)),
        out_shape=[pltpu.VMEM((tall, 2 * width), kind) for kind in kinds],
        in_specs=[vmem] * (2 * len(first)),
        out_specs=[vmem] * last,
        compiler_params=pltpu.CompilerParams(vmem_limit_bytes=4 * 2**20),
        name="join",
    )(*in_vmem(*first, *second))


def finish_kernel(*refs):
    terms, (updates, slots) = refs[:-2], refs[-2:]
    total = add_up([v[...] for v in terms]).astype(jnp.bfloat16)
    steps_count, share, cols = updates.shape
    for t in range(steps_count):
        updates[t] = total[t * share : (t + 1) * share]
    slot = total[steps_count * share :]
    for r in range(slot.shape[0]):
        slots[0:1, r * cols : (r + 1) * cols] = slot[r : r + 1]


def finish(steps_count, terms):
    tall, cols = terms[0].shape
    replicas = lax.axis_size("replica")
    share = (tall - replicas) // steps_count
    vmem = pl.BlockSpec(memory_space=pltpu.VMEM)
    return pl.pallas_call(
        finish_kernel,
        out_shape=(
            jax.ShapeDtypeStruct((steps_count, share, cols), jnp.bfloat16),
            jax.ShapeDtypeStruct((1, replicas * cols), jnp.bfloat16),
        ),
        in_specs=[vmem] * len(terms),
        out_specs=(vmem, vmem),
        compiler_params=pltpu.CompilerParams(vmem_limit_bytes=4 * 2**20),
        name="finish",
    )(*in_vmem(*terms))


def move_sums(
    base_stream,
    out_weight,
    queries,
    cache_keys,
    cache_values,
    new_keys,
    new_values,
    lengths,
    finished,
    owners,
):
    steps_count, row_count, _, _ = queries.shape
    replicas = lax.axis_size("replica")
    model = out_weight.shape[2]
    split = attend_split(queries, cache_keys, cache_values, new_keys, new_values, lengths)
    gathered = lax.all_to_all(split, "replica", split_axis=0, concat_axis=0, tiled=True)
    gathered = gathered.reshape(-1, gathered.shape[2])
    weight = out_weight.reshape(-1, model)
    cols = model // replicas
    half = cols // 2
    calls = ((0, half), (half, half))
    rows, base_rows, *near, rest = select_rows(
        owners, finished, weight, calls, EARLY, steps_count, row_count
    )
    operands = (gathered, rows, base_rows, base_stream)
    core, across = ("tensor", 1), ("tensor", 2)
    beside, along = ("replica", 1), ("replica", 2)
    keep, send = project(calls[0], "xyz", *operands, near[0], near[0])
    first = [keep, exchange(send, *core)]
    keep, send = project(calls[1], "yxz", *operands, near[1], rest)
    second = [keep, exchange(send, *core)]
    first = halve(first, *across)
    first = halve(first, *beside)
    second = halve(second, *beside)
    second = halve(second, *across)
    own, *sends = join(first, second, replicas // 2)
    came = []
    for m, v in enumerate(sends):
        came.append(exchange(v, along[0], along[1] * (m + 1)))
    updates, trainer_rows = finish(steps_count, (own, *came))
    return (updates, trainer_rows.reshape(1, SLOT_DEV, model))


def shards(*arrays):
    out_weight, queries, cache_keys = arrays[1:4]
    steps_count, row_count, heads_here, head_size = queries.shape
    replicas, tensors = lax.axis_size("replica"), lax.axis_size("tensor")
    sent = steps_count * row_count * replicas
    few = sent <= heads_here * out_weight.shape[1]
    group = heads_here // cache_keys.shape[1]
    shares = replicas * row_count // tensors
    powers = all(n & (n - 1) == 0 for n in (replicas, steps_count, row_count, shares))
    fits = tensors == 4 and replicas == group == 8 and powers and head_size == LANES
    fits = fits and out_weight.shape[2] % (replicas * 2 * LANES) == 0
    if not (few and fits):
        return regroup_weight(*arrays)
    return move_sums(*arrays)


def solution(mesh):
    placed = (
        P("tensor", "replica"),
        P("tensor", "replica", None),
        P(None, "replica", "tensor", None),
        P("replica", "tensor", None, None),
        P("replica", "tensor", None, None),
        P(None, "replica", "tensor", None),
        P(None, "replica", "tensor", None),
        P("replica"),
        P(),
        P(),
    )
    return jax.shard_map(
        shards,
        mesh=mesh,
        in_specs=placed,
        out_specs=(P(None, "tensor", "replica"), P("replica", "tensor", None)),
        check_vma=False,
    )
```
